32 devices in a mesh: gz: 2 (over core), row: 4 (over y, x), col: 4 (over z).
Axes of the slice: x: 2, y: 2, z: 4, core: 2. Of those that a mesh axis runs over, the one named last changes fastest.
Arguments:
- right_sides: float32 [32, 4, 16, 256], P(('gz', 'row', 'col')), may hold values from -6 to 6
- lower_inverse: bfloat16 [32, 4, 256, 256], P(('gz', 'row', 'col')), may hold values from -0.375 to 0.375
- upper_inverse: bfloat16 [32, 4, 256, 256], P(('gz', 'row', 'col')), may hold values from -0.375 to 0.375
- lower_blocks: bfloat16 [32, 4, 2, 256, 256], P(('gz', 'row', 'col')), may hold values from -0.125 to 0.125
- upper_blocks: bfloat16 [32, 4, 2, 256, 256], P(('gz', 'row', 'col')), may hold values from -0.125 to 0.125
- node_widths: int32 [32, 4], P(('gz', 'row', 'col')), may hold values from 128 to 256, as said below
- far_levels: int32 [32, 4], P(('gz', 'row', 'col')), may hold values from 0 to 5, as said below
- owner_level: int32 [32], replicated, may hold values from 0 to 5, as said below
Outputs:
- solution: float32 [32, 4, 16, 256], P(('gz', 'row', 'col'))
The draws below stay inside these ranges and needn't reach their ends.
Inputs may be any that keep to these rules, and one draw needn't show every extreme that they name: Columns c >= node_widths of a supernode are padding; every device holds a supernode with all 256 columns. `far_levels`: between 2 and 5 where the supernode has two or more ancestors, but never past the root; 1 where it has one; 0 for the root and for the slot of the device that owns no separator. `owner_level`: every separator of level u is owned by exactly one device of its group (the devices t with the same t // 2**u); one device owns none and holds 0.
All inputs are finite; a program needn't handle non-finite values.
Results may differ from the reference program's by a relative error of at most 0.018.
Values may be sent and summed in bfloat16 or wider, within the bound.
A program may use at most 64 MiB of HBM per device.

```python
import jax
import jax.numpy as jnp

W = 256
RHS = 16
NB = 2
LOCAL_LEVELS = 2
LOCAL_COUNT = 3
NODES = 4
SUBTREES = 32
UPPER = 5
REACH = 5


def owner_table(key):
    free_ids = jnp.arange(SUBTREES, dtype=jnp.int32)
    owned = jnp.zeros((SUBTREES,), jnp.int32)
    count = SUBTREES
    level = 0
    while count > 1:
        level = level + 1
        pairs = free_ids.reshape(count // 2, 2)
        coin = jax.random.randint(jax.random.fold_in(key, 100 + level), (count // 2,), 0, 2)
        chosen = jnp.where(coin == 1, pairs[:, 1], pairs[:, 0])
        staying = jnp.where(coin == 1, pairs[:, 0], pairs[:, 1])
        owned = owned.at[chosen].set(level)
        free_ids = staying
        count = count // 2
    return owned.astype(jnp.int32)


def draw_owner_level(key, part):
    return owner_table(key)


def draw_node_widths(key, part):
    key_one, key_two = jax.random.split(jax.random.fold_in(key, 23))
    widths = jax.random.randint(key_one, (SUBTREES, NODES), W // 2, W + 1)
    full_slot = jax.random.randint(key_two, (SUBTREES, 1), 0, NODES)
    slots = jnp.arange(NODES, dtype=jnp.int32)[None, :]
    return jnp.where(slots == full_slot, W, widths).astype(jnp.int32)


def draw_far_levels(key, part):
    owners = owner_table(key)
    identities = jnp.arange(SUBTREES, dtype=jnp.int32)
    slots = jnp.arange(NODES, dtype=jnp.int32)
    heights = jnp.zeros((NODES,), jnp.int32)
    for step_at in range(LOCAL_LEVELS):
        heights = jnp.where(slots >= 2 ** LOCAL_LEVELS - 2 ** (LOCAL_LEVELS - step_at), step_at, heights)
    local_room = LOCAL_LEVELS - 1 - heights + UPPER
    owned_room = jnp.where(owners > 0, UPPER - owners, 0)
    room_up = jnp.where(slots[None, :] == NODES - 1, owned_room[:, None], local_room[None, :])
    top_reach = jnp.minimum(room_up, REACH)
    random_bits = jax.random.randint(jax.random.fold_in(key, 31), (SUBTREES, NODES), 0, 1 << 20)
    picked = 2 + random_bits % jnp.maximum(top_reach - 1, 1)
    result = jnp.where(room_up >= 2, picked, room_up).astype(jnp.int32)
    group_owner = []
    for level in range(2, UPPER + 1):
        marked = jnp.where(owners == level, identities, 0)
        summed = marked.reshape(SUBTREES // 2 ** level, 2 ** level).sum(axis=1)
        group_owner.append(jnp.repeat(summed, 2 ** level))
    designated = jnp.zeros((SUBTREES,), jnp.int32)
    for index, level in enumerate(range(2, UPPER + 1)):
        holder = group_owner[index]
        beside = (identities == holder + 1) | (identities == holder - 1)
        designated = jnp.where(beside, level, designated)
    for index, level in enumerate(range(2, UPPER + 1)):
        holder = group_owner[index]
        across = identities == jnp.bitwise_xor(holder, 2 ** (level - 1))
        designated = jnp.where(across, level, designated)
    root_slot = (slots == LOCAL_COUNT - 1)[None, :]
    forced = root_slot & (designated[:, None] > 0)
    return jnp.where(forced, designated[:, None], result).astype(jnp.int32)


def steps_of(key, dims, cuts, smallest, high):
    def one(position, blocks):
        steps = jax.random.uniform(jax.random.fold_in(jax.random.fold_in(key, 6), position), (blocks,), jnp.float32, smallest / len(cuts), high / len(cuts))
        return jnp.repeat(jnp.exp(steps), dims[position] // blocks).reshape((-1,) + (1,) * (len(dims) - position - 1))

    factor_of = one(*cuts[0])
    for cut in cuts[1:]:
        factor_of = factor_of * one(*cut)
    return factor_of


def scatter_about(stream_key, dims, spread, bound, shards=(), kind=jnp.bfloat16):
    loudness = steps_of(stream_key, dims, shards, -0.22, 0.18) if shards else 1.0
    drawn = jax.random.normal(stream_key, dims, jnp.float32) * spread * loudness
    return jnp.minimum(jnp.maximum(drawn, -bound), bound).astype(kind)


def setup_inputs(seed: int = 0) -> dict:
    keys = jax.random.split(jax.random.key(seed), 9)
    return {
        "right_sides": scatter_about(keys[0], (SUBTREES, NODES, RHS, W), 1.0, 6.0, ((0, 32),), jnp.float32),
        "lower_inverse": scatter_about(keys[1], (SUBTREES, NODES, W, W), W ** -0.5, 0.375, ((0, 32),)),
        "upper_inverse": scatter_about(keys[2], (SUBTREES, NODES, W, W), W ** -0.5, 0.375, ((0, 32),)),
        "lower_blocks": scatter_about(keys[3], (SUBTREES, NODES, NB, W, W), (8 * W) ** -0.5, 0.125, ((0, 32),)),
        "upper_blocks": scatter_about(keys[4], (SUBTREES, NODES, NB, W, W), (8 * W) ** -0.5, 0.125, ((0, 32),)),
        "node_widths": draw_node_widths(jax.random.fold_in(keys[8], 71), 0),
        "far_levels": draw_far_levels(jax.random.fold_in(keys[8], 71), 0),
        "owner_level": draw_owner_level(jax.random.fold_in(keys[8], 71), 0),
    }


def level_start(height):
    return 2 ** LOCAL_LEVELS - 2 ** (LOCAL_LEVELS - height)


def apply_blocks(vectors, blocks):
    return jnp.einsum("snrk,snak->snra", vectors.astype(jnp.float32), blocks.astype(jnp.float32))


def apply_single(vectors, blocks):
    return jnp.einsum("srk,sak->sra", vectors.astype(jnp.float32), blocks.astype(jnp.float32))


def forward_local(right_sides, lower_inverse, lower_blocks, padding, far_levels, upper_levels):
    batch_size = right_sides.shape[0]
    pending = jnp.zeros((batch_size, LOCAL_COUNT, RHS, W), jnp.float32)
    upper_pending = jnp.zeros((batch_size, upper_levels, RHS, W), jnp.float32)
    solved = []
    for height in range(LOCAL_LEVELS):
        offset = level_start(height)
        amount = 2 ** (LOCAL_LEVELS - 1 - height)
        residue = (right_sides[:, offset:offset + amount] - pending[:, offset:offset + amount]).astype(jnp.bfloat16)
        solved_now = padding[:, offset:offset + amount] * apply_blocks(residue, lower_inverse[:, offset:offset + amount])
        solved.append(solved_now)
        rounded = solved_now.astype(jnp.bfloat16)
        for block_id in range(NB):
            product = apply_blocks(rounded, lower_blocks[:, offset:offset + amount, block_id])
            for distance in range(1, REACH + 1):
                if block_id == 0 and distance > 1:
                    continue
                if block_id == 0:
                    chosen = product
                else:
                    matches = far_levels[:, offset:offset + amount] == distance
                    chosen = jnp.where(matches[:, :, None, None], product, 0.0)
                target = height + distance
                if target < LOCAL_LEVELS:
                    target_count = amount // 2 ** distance
                    folded = chosen.reshape(batch_size, target_count, 2 ** distance, RHS, W).sum(axis=2)
                    begin_at = level_start(target)
                    pending = pending.at[:, begin_at:begin_at + target_count].add(folded)
                elif target - LOCAL_LEVELS < upper_levels:
                    upper_pending = upper_pending.at[:, target - LOCAL_LEVELS].add(chosen.sum(axis=1))
    return jnp.concatenate(solved, axis=1), upper_pending


def backward_local(forward, upper_inverse, upper_blocks, padding, far_levels, upper_known):
    upper_levels = upper_known.shape[1]
    solutions = [None] * LOCAL_LEVELS
    for height in reversed(range(LOCAL_LEVELS)):
        offset = level_start(height)
        amount = 2 ** (LOCAL_LEVELS - 1 - height)
        residue = forward[:, offset:offset + amount]
        for block_id in range(NB):
            operand = jnp.zeros(residue.shape, jnp.float32)
            for distance in range(1, REACH + 1):
                if block_id == 0 and distance > 1:
                    continue
                target = height + distance
                if target < LOCAL_LEVELS:
                    known_part = jnp.repeat(solutions[target], 2 ** distance, axis=1)
                elif target - LOCAL_LEVELS < upper_levels:
                    known_part = jnp.broadcast_to(upper_known[:, target - LOCAL_LEVELS][:, None], residue.shape)
                else:
                    continue
                if block_id == 0:
                    operand = known_part
                else:
                    matches = far_levels[:, offset:offset + amount] == distance
                    operand = operand + jnp.where(matches[:, :, None, None], known_part, 0.0)
            residue = residue - apply_blocks(operand.astype(jnp.bfloat16), upper_blocks[:, offset:offset + amount, block_id])
        solutions[height] = padding[:, offset:offset + amount] * apply_blocks(residue.astype(jnp.bfloat16), upper_inverse[:, offset:offset + amount])
    return jnp.concatenate(solutions, axis=1)


def reference(right_sides, lower_inverse, upper_inverse, lower_blocks, upper_blocks, node_widths, far_levels, owner_level):
    upper_levels = UPPER
    columns = jnp.arange(W, dtype=jnp.int32)
    padding = (columns[None, None, None, :] < node_widths[:, :, None, None]).astype(jnp.float32)
    forward_nodes, upper_pending = forward_local(
        right_sides[:, :LOCAL_COUNT], lower_inverse[:, :LOCAL_COUNT], lower_blocks[:, :LOCAL_COUNT],
        padding[:, :LOCAL_COUNT], far_levels[:, :LOCAL_COUNT], upper_levels)
    own_rights = right_sides[:, LOCAL_COUNT]
    own_padding = padding[:, LOCAL_COUNT]
    own_far = far_levels[:, LOCAL_COUNT]
    own_forward = jnp.zeros((SUBTREES, RHS, W), jnp.float32)
    for height in range(1, upper_levels + 1):
        group_size = 2 ** height
        totals = upper_pending[:, height - 1].reshape(SUBTREES // group_size, group_size, RHS, W).sum(axis=1)
        gathered = jnp.repeat(totals, group_size, axis=0)
        owner_here = (owner_level == height)[:, None, None]
        residue = (own_rights - gathered).astype(jnp.bfloat16)
        solved_now = jnp.where(owner_here, own_padding * apply_single(residue, lower_inverse[:, LOCAL_COUNT]), 0.0)
        own_forward = own_forward + solved_now
        rounded = solved_now.astype(jnp.bfloat16)
        for block_id in range(NB):
            product = apply_single(rounded, lower_blocks[:, LOCAL_COUNT, block_id])
            for distance in range(1, REACH + 1):
                if block_id == 0 and distance > 1:
                    continue
                target = height + distance
                if target > upper_levels:
                    continue
                if block_id == 0:
                    chosen = product
                else:
                    chosen = jnp.where((own_far == distance)[:, None, None], product, 0.0)
                upper_pending = upper_pending.at[:, target - 1].add(chosen)
    upper_known = jnp.zeros((SUBTREES, upper_levels, RHS, W), jnp.float32)
    own_solution = jnp.zeros((SUBTREES, RHS, W), jnp.float32)
    for height in range(upper_levels, 0, -1):
        group_size = 2 ** height
        owner_here = (owner_level == height)[:, None, None]
        residue = own_forward
        for block_id in range(NB):
            operand = jnp.zeros((SUBTREES, RHS, W), jnp.float32)
            for distance in range(1, REACH + 1):
                if block_id == 0 and distance > 1:
                    continue
                target = height + distance
                if target > upper_levels:
                    continue
                known_part = upper_known[:, target - 1]
                if block_id == 0:
                    operand = known_part
                else:
                    operand = operand + jnp.where((own_far == distance)[:, None, None], known_part, 0.0)
            residue = residue - apply_single(operand.astype(jnp.bfloat16), upper_blocks[:, LOCAL_COUNT, block_id])
        solved_now = jnp.where(owner_here, own_padding * apply_single(residue.astype(jnp.bfloat16), upper_inverse[:, LOCAL_COUNT]), 0.0)
        own_solution = own_solution + solved_now
        totals = solved_now.reshape(SUBTREES // group_size, group_size, RHS, W).sum(axis=1)
        upper_known = upper_known.at[:, height - 1].set(jnp.repeat(totals, group_size, axis=0))
    local_solution = backward_local(
        forward_nodes, upper_inverse[:, :LOCAL_COUNT], upper_blocks[:, :LOCAL_COUNT],
        padding[:, :LOCAL_COUNT], far_levels[:, :LOCAL_COUNT], upper_known)
    return jnp.concatenate([local_solution, own_solution[:, None]], axis=1)
```

```python
import functools

import jax
import jax.numpy as jnp
from jax import lax
from jax.experimental import pallas as pl
from jax.experimental.pallas import tpu as pltpu
from jax.sharding import PartitionSpec as P

W = 256
RHS = 16
NB = 2
LOCAL_LEVELS = 2
LOCAL_COUNT = 3
OWN = LOCAL_COUNT
AXES = ("gz", "row", "col")


def flip_bits(coord, mask):
    flipped = coord
    bit = 1
    while bit <= mask:
        if mask & bit:
            flipped = flipped + bit - 2 * bit * lax.rem(lax.div(coord, bit), 2)
        bit *= 2
    return flipped


def exchange_plan(level, low=0):
    phases = []
    while low < level:
        high = min(low + 4, level)
        phases.append([step << low for step in range((1 << (high - low)) - 1, 0, -1)])
        low = high
    return phases


def times(vectors, matrix):
    return lax.dot_general(
        vectors, matrix, (((1,), (1,)), ((), ())), preferred_element_type=jnp.float32
    )


def half(values):
    return values.astype(jnp.bfloat16)


HANDOUT = {
    2: ((1, False, 0),),
    3: ((2, False, 0), (1, False, 1)),
    4: ((2, False, 1), (1, True, 0)),
    5: ((1, True, 1),),
}
NEAR_BITS = 2
NEAR = 2**NEAR_BITS
CHAIN, TOP_SOLVE, SUB_SOLVE, BACK = range(4)
SOURCES = {CHAIN: 0, TOP_SOLVE: 1, SUB_SOLVE: 1, BACK: 2}


def kernel(
    spans,
    plans,
    down_plans,
    rights_hbm,
    lower_inverse_hbm,
    upper_inverse_hbm,
    lower_blocks_hbm,
    upper_blocks_hbm,
    widths_ref,
    far_ref,
    owner_ref,
    out_ref,
    rights,
    lower_inverse,
    upper_inverse,
    lower_blocks,
    upper_blocks,
    outgoing,
    incoming,
    fused,
    replicas,
    fars,
    bases,
    scattered,
    doubled,
    whole,
    load_sems,
    send_sems,
    recv_sems,
    bulk_send_sems,
    bulk_recv_sems,
    spread_send_sems,
    spread_recv_sems,
):
    layer_span, row_span, col_span = spans
    col_bits = col_span.bit_length() - 1
    layer_size = row_span * col_span
    upper_levels = len(plans)
    top, sub = upper_levels, upper_levels - 1
    layer_at = lax.axis_index("gz")
    row_at = lax.axis_index("row")
    col_at = lax.axis_index("col")
    device = (layer_at * row_span + row_at) * col_span + col_at

    def peer(offset):
        return (
            flip_bits(layer_at, offset // layer_size),
            flip_bits(row_at, offset // col_span % row_span),
            flip_bits(col_at, offset % col_span),
        )

    pieces = [
        (rights_hbm.at[0], rights),
        (lower_inverse_hbm.at[0, pl.ds(0, 2)], lower_inverse.at[pl.ds(0, 2)]),
        (lower_blocks_hbm.at[0, pl.ds(0, 2)], lower_blocks.at[pl.ds(0, 2)]),
        (lower_inverse_hbm.at[0, pl.ds(2, 2)], lower_inverse.at[pl.ds(2, 2)]),
        (lower_blocks_hbm.at[0, pl.ds(2, 2)], lower_blocks.at[pl.ds(2, 2)]),
        (upper_blocks_hbm.at[0], upper_blocks),
        (upper_inverse_hbm.at[0], upper_inverse),
    ]
    loads = [
        pltpu.make_async_copy(source, target, load_sems.at[at])
        for at, (source, target) in enumerate(pieces)
    ]
    for load in loads:
        load.start()

    barrier = pltpu.get_barrier_semaphore()
    partners = sorted({offset for plan in plans for phase in plan for offset in phase})
    for offset in partners:
        pl.semaphore_signal(
            barrier, inc=1, device_id=peer(offset), device_id_type=pl.DeviceIdType.MESH
        )

    columns = lax.broadcasted_iota(jnp.int32, (RHS, W), 1)

    def spread(scalar):
        return jnp.full((RHS, W), scalar, jnp.int32)

    inside = [columns < widths_ref[0, slot] for slot in range(LOCAL_COUNT + 1)]
    far = [spread(far_ref[0, slot]) for slot in range(LOCAL_COUNT + 1)]
    my_level = spread(owner_ref[device])
    zeros = jnp.zeros((RHS, W), jnp.float32)

    steps = []
    for bit in range(upper_levels):
        size = 1 << bit
        steps.append(size - 2 * size * lax.rem(lax.div(device, size), 2))

    def level_at(offset):
        at = device
        for bit in range(upper_levels):
            if offset >> bit & 1:
                at = at + steps[bit]
        return owner_ref[at]

    def padded(slot, values):
        return jnp.where(inside[slot], values, 0.0)

    counts = [0, 0, 0]
    sends = []

    def launch(rounded, phase):
        outbox, amount = counts[0], len(rounded)
        counts[0] += amount
        for index, part in enumerate(rounded):
            outgoing[outbox + index] = part
        copies = []
        for offset in phase:
            at, message = counts[1], counts[2]
            counts[1] += amount
            counts[2] += 1
            copy = pltpu.make_async_remote_copy(
                src_ref=outgoing.at[pl.ds(outbox, amount)],
                dst_ref=incoming.at[pl.ds(at, amount)],
                send_sem=send_sems.at[message],
                recv_sem=recv_sems.at[message],
                device_id=peer(offset),
                device_id_type=pl.DeviceIdType.MESH,
            )
            copy.start()
            copies.append((copy, at))
        sends.extend(copies)
        return copies

    bulk = {}

    def hand_out(name, source, target, offset):
        at = len(bulk)
        bulk[name] = pltpu.make_async_remote_copy(
            src_ref=source,
            dst_ref=target,
            send_sem=bulk_send_sems.at[at],
            recv_sem=bulk_recv_sems.at[at],
            device_id=peer(offset),
            device_id_type=pl.DeviceIdType.MESH,
        )
        bulk[name].start()

    received = set()

    def await_bulk(name):
        if name not in received:
            received.add(name)
            bulk[name].wait_recv()

    def exchange(values, plan, narrow, besides):
        for index, phase in enumerate(plan):
            rounded = [half(value) for value in values]
            copies = launch(rounded, phase)
            if index < len(besides):
                besides[index]()
            if narrow:
                values = [part.astype(jnp.float32) for part in rounded]
            for copy, at in copies:
                copy.wait_recv()
                values = [
                    value + incoming[at + part].astype(jnp.float32)
                    for part, value in enumerate(values)
                ]
        return values

    strip = W // row_span
    my_strip = pl.ds(pl.multiple_of(row_at * strip, strip), strip)
    stream_level = {CHAIN: sub, TOP_SOLVE: top, SUB_SOLVE: sub, BACK: sub}
    spreads = []
    spread_waits = {}

    def spread_copy(key, source, target, offset):
        at = len(spreads)
        copy = pltpu.make_async_remote_copy(
            src_ref=source,
            dst_ref=target,
            send_sem=spread_send_sems.at[at],
            recv_sem=spread_recv_sems.at[at],
            device_id=peer(offset),
            device_id_type=pl.DeviceIdType.MESH,
        )
        copy.start()
        spreads.append(copy)
        spread_waits.setdefault(key, []).append(copy)

    def await_spread(key):
        for copy in spread_waits.pop(key, ()):
            copy.wait_recv()

    held = {}
    for level in (sub, top):
        plane = []
        place = jnp.int32(0)
        for step in range(row_span):
            found = [
                level_at(step * col_span + offset) == level for offset in range(col_span)
            ]
            place = jnp.where(found[0], step, place)
            plane.append(found)
        known_here = []
        for bit in range(col_bits + 1):
            here = jnp.int32(1)
            for found in plane:
                for offset in range(1 << bit):
                    here = jnp.where(found[offset], 0, here)
            known_here.append(here)
        held[level] = (place, known_here)

    def scatter_rows(source, matrix):
        for step in range(1, row_span):
            start = pl.multiple_of(flip_bits(row_at, step) * strip, strip)
            spread_copy(
                ("scatter", source),
                matrix.at[pl.ds(start, strip)],
                scattered[source].at[step],
                step * col_span,
            )
        scattered[source][0] = matrix[my_strip]

    def merged(stream, stage):
        place, known_here = held[stream_level[stream]]
        if stage == 0:
            await_spread(("scatter", SOURCES[stream]))
            return scattered[SOURCES[stream]][place]
        await_spread(("double", stream, stage - 1))
        return doubled[stream][stage - 1][known_here[stage - 1]]

    def double_cols(stream, stage):
        doubled[stream][stage][0] = merged(stream, stage)
        spread_copy(
            ("double", stream, stage),
            doubled[stream][stage].at[0],
            doubled[stream][stage].at[1],
            1 << stage if stage < col_bits else layer_size,
        )

    def gather_rows(stream, stage):
        whole[stream][my_strip] = merged(stream, stage)
        for step in range(1, row_span):
            spread_copy(
                ("gather", stream),
                whole[stream].at[my_strip],
                whole[stream].at[my_strip],
                step * col_span,
            )

    pending = [None] + [zeros for _ in range(upper_levels)]

    def scatter_up(product, slot, height):
        for level in range(1, upper_levels + 1):
            pending[level] = pending[level] + jnp.where(
                far[slot] == level + LOCAL_LEVELS - 1 - height, product, 0.0
            )

    forward = [None] * (LOCAL_COUNT + 1)
    loads[0].wait()
    loads[1].wait()
    for slot in range(2):
        forward[slot] = padded(slot, times(half(rights[slot]), lower_inverse[slot]))
    loads[2].wait()
    near = times(half(forward[0]), lower_blocks[0, 0]) + times(
        half(forward[1]), lower_blocks[1, 0]
    )
    for slot in range(2):
        scatter_up(times(half(forward[slot]), lower_blocks[slot, 1]), slot, 0)
    loads[3].wait()
    loads[4].wait()
    forward[2] = padded(2, times(half(rights[2] - near), lower_inverse[2]))
    pending[1] = pending[1] + times(half(forward[2]), lower_blocks[2, 0])
    scatter_up(times(half(forward[2]), lower_blocks[2, 1]), 2, 1)
    for level in (sub, top):
        pending[level] = pending[level] - jnp.where(my_level == level, rights[OWN], 0.0)

    pl.semaphore_wait(barrier, len(partners))

    wide_columns = lax.broadcasted_iota(jnp.int32, (W, W), 1)
    wide_rows = lax.broadcasted_iota(jnp.int32, (W, W), 0)

    def own_columns(matrix):
        kept = jnp.where(
            wide_columns < widths_ref[0, OWN], matrix.astype(jnp.float32), 0.0
        )
        return half(kept)

    def own_rows(matrix):
        return jnp.where(wide_rows < widths_ref[0, OWN], matrix, 0.0)

    def lower_product(block_id):
        return jnp.dot(
            own_columns(lower_blocks[OWN, block_id]),
            lower_inverse[OWN],
            preferred_element_type=jnp.float32,
        )

    def upper_product(slot, block_id):
        return jnp.dot(
            upper_inverse[slot], upper_blocks[slot, block_id], preferred_element_type=jnp.float32
        )

    def split_times(values, matrix):
        large = half(values)
        small = half(values - large.astype(jnp.float32))
        return times(large, matrix) + times(small, matrix)

    far_is_near = jnp.full((W, W), far_ref[0, OWN], jnp.int32) == 1

    own_base = [zeros]
    residue = [None]

    def own_solve(level):
        solved = times(residue[0], fused[2])
        own_base[0] = own_base[0] + jnp.where(my_level == level, solved, 0.0)

    def far_up(level):
        product = jnp.where(my_level == level, times(residue[0], fused[1]), 0.0)
        for target in range(level + 2, upper_levels + 1):
            pending[target] = pending[target] + jnp.where(
                far[OWN] == target - level, product, 0.0
            )

    def hand_out_row(slot_of):
        for offset, relayed, block_id in HANDOUT.get(slot_of, ()):
            kept = 2 if relayed else 0
            if relayed:
                await_bulk((2, False, block_id))
            hand_out(
                (offset, relayed, block_id),
                replicas.at[kept, block_id],
                replicas.at[kept + offset, block_id],
                offset,
            )

    def leaf_products(slot):
        for block_id in range(NB):
            fused[3 + 2 * slot + block_id] = half(upper_product(slot, block_id))

    leaf_base = [None] * LOCAL_COUNT

    def beside_up(level):
        if level == 1:
            fars[0] = far[OWN][: fars.shape[1], : fars.shape[2]].astype(jnp.float32)
            for offset in range(1, NEAR):
                hand_out(("far", offset), fars.at[0], fars.at[offset], offset)
            far_product = lower_product(1)
            fused[0] = half(lower_product(0) + jnp.where(far_is_near, far_product, 0.0))
            scatter_rows(0, fused.at[0])
            fused[1] = half(far_product)
            loads[5].wait()
            loads[6].wait()
            fused[2] = half(
                own_rows(
                    jnp.dot(
                        own_columns(upper_inverse[OWN]),
                        lower_inverse[OWN],
                        preferred_element_type=jnp.float32,
                    )
                )
            )
            scatter_rows(1, fused.at[2])
            far_product = own_rows(upper_product(OWN, 1))
            replicas[0, 1] = half(far_product)
            replicas[0, 0] = half(
                own_rows(upper_product(OWN, 0)) + jnp.where(far_is_near, far_product, 0.0)
            )
            scatter_rows(2, replicas.at[0, 0])
            return
        if level < sub:
            far_up(level - 1)
        own_solve(level - 1)
        if level < sub:
            for stream in (CHAIN, TOP_SOLVE, SUB_SOLVE):
                double_cols(stream, level - 2)
            if level > 2:
                double_cols(BACK, level - 3)
        hand_out_row(level)
        if level - 2 < LOCAL_COUNT:
            leaf_products(level - 2)

    def beside_sub(index):
        if index == 0:
            bases[0] = own_base[0]
            for offset in reversed(range(1, NEAR)):
                hand_out(("base", offset), bases.at[0], bases.at[offset], offset)
            double_cols(TOP_SOLVE, col_bits)
            gather_rows(CHAIN, col_bits)
            gather_rows(SUB_SOLVE, col_bits)
            double_cols(BACK, col_bits - 1)
        if index == len(plans[sub - 1]) - 1:
            gather_rows(TOP_SOLVE, col_bits + 1)
            gather_rows(BACK, col_bits)
            hand_out_row(sub + 1)

    for level in range(1, sub):
        gathered = exchange(
            [pending[level]], plans[level - 1], False, [functools.partial(beside_up, level)]
        )[0]
        residue[0] = half(rights[OWN] - gathered)
        product = times(residue[0], fused[0])
        pending[level + 1] = pending[level + 1] + jnp.where(my_level == level, product, 0.0)
    far_up(sub - 1)

    def first_beside():
        beside_up(sub)
        beside_sub(0)

    sums = exchange(
        [pending[sub], pending[top]],
        plans[sub - 1],
        False,
        [first_beside]
        + [functools.partial(beside_sub, index) for index in range(1, len(plans[sub - 1]))],
    )
    sub_residue = half(-sums[0])
    await_spread(("gather", CHAIN))
    layer_sum = sums[1] + times(sub_residue, whole[CHAIN][...])
    sub_base = [None]

    def beside_top():
        await_spread(("gather", SUB_SOLVE))
        sub_base[0] = times(sub_residue, whole[SUB_SOLVE][...])
        for slot in range(LOCAL_COUNT):
            leaf_base[slot] = split_times(forward[slot], upper_inverse[slot])
        await_spread(("gather", TOP_SOLVE))
        await_spread(("gather", BACK))

    total = exchange([layer_sum], plans[top - 1], False, [beside_top])[0]

    known = [None] * (upper_levels + 1)

    def pick(slot, below, lowest):
        chosen = zeros
        for level in range(lowest, upper_levels + 1):
            chosen = chosen + jnp.where(far[slot] == level - below, known[level], 0.0)
        return half(chosen)

    far_part = [zeros]
    near_levels = [level_at(offset) for offset in range(NEAR)]

    def holder(level):
        offset_of = jnp.int32(0)
        found = jnp.int32(0)
        for offset in range(min(NEAR, 2**level)):
            offset_of = jnp.where(near_levels[offset] == level, offset, offset_of)
            found = jnp.where(near_levels[offset] == level, 1, found)
        return offset_of, found

    def prepare(level):
        if level < 1 or level + 2 > upper_levels:
            return
        at, _ = holder(level)
        reach = fars[at]
        reach = jnp.concatenate([reach] * (W // reach.shape[1]), axis=1)
        reach = jnp.concatenate([reach] * (RHS // reach.shape[0]), axis=0)
        chosen = zeros
        for target in range(level + 2, upper_levels + 1):
            chosen = chosen + jnp.where(reach == float(target - level), known[target], 0.0)
        far_part[0] = times(half(chosen), replicas[at, 1])

    solved = times(half(-total), whole[TOP_SOLVE][...])
    own_solution = jnp.where(my_level == top, solved, 0.0)
    known[top] = half(solved).astype(jnp.float32)
    solved = sub_base[0] - times(half(solved), whole[BACK][...])
    own_solution = own_solution + jnp.where(my_level == sub, solved, 0.0)
    known[sub] = half(solved).astype(jnp.float32)
    for name in bulk:
        await_bulk(name)
    prepare(sub - 1)

    for level in range(sub - 1, 0, -1):
        at, found = holder(level)
        solved = bases[at] - far_part[0] - times(half(known[level + 1]), replicas[at, 0])
        solved = jnp.where(spread(found) == 1, solved, 0.0)
        own_solution = own_solution + jnp.where(my_level == level, solved, 0.0)
        if down_plans[level - 1]:
            known[level] = exchange(
                [solved], down_plans[level - 1], True, [functools.partial(prepare, level - 1)]
            )[0]
        else:
            known[level] = half(solved).astype(jnp.float32)
            prepare(level - 1)
    leaf_base[2] = leaf_base[2] - times(pick(2, 0, 2), fused[3 + 2 * 2 + 1])
    out_ref[0, OWN] = own_solution

    nearest = half(known[1])
    root = padded(2, leaf_base[2] - times(nearest, fused[3 + 2 * 2]))
    out_ref[0, 2] = root
    for slot in range(2):
        solved = leaf_base[slot] - times(pick(slot, -1, 1), fused[3 + 2 * slot + 1])
        solved = solved - times(half(root), fused[3 + 2 * slot])
        out_ref[0, slot] = padded(slot, solved)

    for copy, _ in sends:
        copy.wait_send()
    for copy in bulk.values():
        copy.wait_send()
    for copy in spreads:
        copy.wait_send()


def local(
    spans,
    right_sides,
    lower_inverse,
    upper_inverse,
    lower_blocks,
    upper_blocks,
    node_widths,
    far_levels,
    owner_level,
):
    layer_span, row_span, col_span = spans
    upper_levels = (layer_span * row_span * col_span).bit_length() - 1
    row_bits, col_bits = row_span.bit_length() - 1, col_span.bit_length() - 1
    top, sub = upper_levels, upper_levels - 1
    plans = [exchange_plan(level) for level in range(1, sub)]
    plans.append(exchange_plan(col_bits) + exchange_plan(sub, col_bits))
    plans.append(exchange_plan(top, sub))
    down_plans = [exchange_plan(level, NEAR_BITS) for level in range(1, sub)]
    vectors = [1] * (sub - 1) + [2, 1] + [1] * len(down_plans)
    routes = list(zip(vectors, plans + down_plans))
    phases = sum(amount * len(plan) for amount, plan in routes)
    messages = sum(len(phase) for _, plan in routes for phase in plan)
    boxes = sum(amount * len(phase) for amount, plan in routes for phase in plan)
    handed = 2 * (NEAR - 1) + sum(len(row) for row in HANDOUT.values())
    streams, sources = len(SOURCES), len(set(SOURCES.values()))
    strip = W // row_span
    spread_count = (sources + streams) * (row_span - 1) + streams * col_bits + 1
    hbm = pl.BlockSpec(memory_space=pl.ANY)
    smem = pl.BlockSpec(memory_space=pltpu.SMEM)
    return pl.pallas_call(
        functools.partial(kernel, spans, plans, down_plans),
        out_shape=jax.ShapeDtypeStruct(right_sides.shape, jnp.float32),
        in_specs=[hbm] * 5 + [smem] * 3,
        out_specs=pl.BlockSpec(memory_space=pltpu.VMEM),
        scratch_shapes=[
            pltpu.VMEM(right_sides.shape[1:], jnp.float32),
            pltpu.VMEM(lower_inverse.shape[1:], jnp.bfloat16),
            pltpu.VMEM(upper_inverse.shape[1:], jnp.bfloat16),
            pltpu.VMEM(lower_blocks.shape[1:], jnp.bfloat16),
            pltpu.VMEM(upper_blocks.shape[1:], jnp.bfloat16),
            pltpu.VMEM((phases, RHS, W), jnp.bfloat16),
            pltpu.VMEM((boxes, RHS, W), jnp.bfloat16),
            pltpu.VMEM((3 + NB * LOCAL_COUNT, W, W), jnp.bfloat16),
            pltpu.VMEM((NEAR, NB, W, W), jnp.bfloat16),
            pltpu.VMEM((NEAR, 8, 128), jnp.float32),
            pltpu.VMEM((NEAR, RHS, W), jnp.float32),
            [pltpu.VMEM((row_span, strip, W), jnp.bfloat16)] * sources,
            [[pltpu.VMEM((2, strip, W), jnp.bfloat16)] * (col_bits + 1)] * streams,
            [pltpu.VMEM((W, W), jnp.bfloat16)] * streams,
            pltpu.SemaphoreType.DMA((7,)),
            pltpu.SemaphoreType.DMA((messages,)),
            pltpu.SemaphoreType.DMA((messages,)),
            pltpu.SemaphoreType.DMA((handed,)),
            pltpu.SemaphoreType.DMA((handed,)),
            pltpu.SemaphoreType.DMA((spread_count,)),
            pltpu.SemaphoreType.DMA((spread_count,)),
        ],
        compiler_params=pltpu.CompilerParams(collective_id=0, has_side_effects=True),
        name="tree_solve",
    )(
        right_sides,
        lower_inverse,
        upper_inverse,
        lower_blocks,
        upper_blocks,
        node_widths,
        far_levels,
        owner_level,
    )


def solution(mesh):
    spans = tuple(mesh.shape[axis] for axis in AXES)
    split = P(AXES)
    return jax.shard_map(
        functools.partial(local, spans),
        mesh=mesh,
        in_specs=(split,) * 7 + (P(),),
        out_specs=split,
        check_vma=False,
    )
```

```python
import functools

import jax
import jax.numpy as jnp
from jax import lax
from jax.experimental import pallas as pl
from jax.experimental.pallas import tpu as pltpu
from jax.sharding import PartitionSpec as P

W = 256
RHS = 16
NB = 2
LOCAL_LEVELS = 2
LOCAL_COUNT = 3
OWN = LOCAL_COUNT
AXES = ("gz", "row", "col")


def flip_bits(coord, mask):
    flipped = coord
    bit = 1
    while bit <= mask:
        if mask & bit:
            flipped = flipped + bit - 2 * bit * lax.rem(lax.div(coord, bit), 2)
        bit *= 2
    return flipped


def exchange_plan(bits):
    phases = []
    for low in range(0, len(bits), 4):
        offsets = [0]
        for bit in bits[low : low + 4]:
            offsets += [offset + (1 << bit) for offset in offsets]
        phases.append(offsets[:0:-1])
    return phases


def times(vectors, matrix):
    return lax.dot_general(
        vectors, matrix, (((1,), (1,)), ((), ())), preferred_element_type=jnp.float32
    )


def half(values):
    return values.astype(jnp.bfloat16)


NEAR_BITS = 2
NEAR = 2**NEAR_BITS
CHAIN, TOP_SOLVE, SUB_SOLVE, BACK = range(4)
SOURCES = {CHAIN: 0, TOP_SOLVE: 1, SUB_SOLVE: 1, BACK: 2}


def kernel(
    spans,
    plans,
    down_plans,
    rights_hbm,
    lower_inverse_hbm,
    upper_inverse_hbm,
    lower_blocks_hbm,
    upper_blocks_hbm,
    widths_ref,
    far_ref,
    owner_ref,
    out_ref,
    rights,
    lower_inverse,
    upper_inverse,
    lower_blocks,
    upper_blocks,
    outgoing,
    incoming,
    fused,
    near_blocks,
    far_blocks,
    second,
    beside_near,
    beside_far,
    fars,
    bases,
    scattered,
    doubled,
    whole,
    load_sems,
    send_sems,
    recv_sems,
    bulk_send_sems,
    bulk_recv_sems,
    spread_send_sems,
    spread_recv_sems,
):
    layer_span, row_span, col_span = spans
    col_bits = col_span.bit_length() - 1
    layer_size = row_span * col_span
    upper_levels = len(plans)
    top, sub = upper_levels, upper_levels - 1
    layer_at = lax.axis_index("gz")
    row_at = lax.axis_index("row")
    col_at = lax.axis_index("col")
    device = (layer_at * row_span + row_at) * col_span + col_at

    def peer(offset):
        return (
            flip_bits(layer_at, offset // layer_size),
            flip_bits(row_at, offset // col_span % row_span),
            flip_bits(col_at, offset % col_span),
        )

    pieces = [
        (rights_hbm.at[0], rights),
        (lower_inverse_hbm.at[0, pl.ds(0, 2)], lower_inverse.at[pl.ds(0, 2)]),
        (lower_blocks_hbm.at[0, pl.ds(0, 2)], lower_blocks.at[pl.ds(0, 2)]),
        (lower_inverse_hbm.at[0, pl.ds(2, 2)], lower_inverse.at[pl.ds(2, 2)]),
        (lower_blocks_hbm.at[0, pl.ds(2, 2)], lower_blocks.at[pl.ds(2, 2)]),
        (upper_blocks_hbm.at[0], upper_blocks),
        (upper_inverse_hbm.at[0], upper_inverse),
    ]
    loads = [
        pltpu.make_async_copy(source, target, load_sems.at[at])
        for at, (source, target) in enumerate(pieces)
    ]
    for load in loads:
        load.start()

    barrier = pltpu.get_barrier_semaphore()
    partners = {offset for plan in plans for phase in plan for offset in phase}
    partners = sorted(partners | {step * col_span for step in range(1, row_span)})
    for offset in partners:
        pl.semaphore_signal(
            barrier, inc=1, device_id=peer(offset), device_id_type=pl.DeviceIdType.MESH
        )

    columns = lax.broadcasted_iota(jnp.int32, (RHS, W), 1)

    def spread(scalar):
        return jnp.full((RHS, W), scalar, jnp.int32)

    inside = [columns < widths_ref[0, slot] for slot in range(LOCAL_COUNT + 1)]
    far = [spread(far_ref[0, slot]) for slot in range(LOCAL_COUNT + 1)]
    my_level_scalar = owner_ref[device]
    my_level = spread(my_level_scalar)
    zeros = jnp.zeros((RHS, W), jnp.float32)

    steps = []
    for bit in range(upper_levels):
        size = 1 << bit
        steps.append(size - 2 * size * lax.rem(lax.div(device, size), 2))

    def level_at(offset):
        at = device
        for bit in range(upper_levels):
            if offset >> bit & 1:
                at = at + steps[bit]
        return owner_ref[at]

    def padded(slot, values):
        return jnp.where(inside[slot], values, 0.0)

    counts = [0, 0, 0]
    sends = []

    def launch(rounded, phase):
        outbox, amount = counts[0], len(rounded)
        counts[0] += amount
        for index, part in enumerate(rounded):
            outgoing[outbox + index] = part
        copies = []
        for offset in phase:
            at, message = counts[1], counts[2]
            counts[1] += amount
            counts[2] += 1
            copy = pltpu.make_async_remote_copy(
                src_ref=outgoing.at[pl.ds(outbox, amount)],
                dst_ref=incoming.at[pl.ds(at, amount)],
                send_sem=send_sems.at[message],
                recv_sem=recv_sems.at[message],
                device_id=peer(offset),
                device_id_type=pl.DeviceIdType.MESH,
            )
            copy.start()
            copies.append((copy, at))
        sends.extend(copies)
        return copies

    bulk = {}

    def hand_out(name, source, target, offset):
        at = len(bulk)
        bulk[name] = pltpu.make_async_remote_copy(
            src_ref=source,
            dst_ref=target,
            send_sem=bulk_send_sems.at[at],
            recv_sem=bulk_recv_sems.at[at],
            device_id=peer(offset),
            device_id_type=pl.DeviceIdType.MESH,
        )
        bulk[name].start()

    received = set()

    def await_bulk(name):
        if name not in received:
            received.add(name)
            bulk[name].wait_recv()

    def exchange(values, plan, narrow, besides):
        for index, phase in enumerate(plan):
            rounded = [half(value) for value in values]
            copies = launch(rounded, phase)
            if index < len(besides):
                besides[index]()
            if narrow:
                values = [part.astype(jnp.float32) for part in rounded]
            for copy, at in copies:
                copy.wait_recv()
                values = [
                    value + incoming[at + part].astype(jnp.float32)
                    for part, value in enumerate(values)
                ]
        return values

    strip = W // row_span
    my_strip = pl.ds(pl.multiple_of(row_at * strip, strip), strip)
    stream_level = {CHAIN: sub, TOP_SOLVE: top, SUB_SOLVE: sub, BACK: sub}
    spreads = []
    spread_waits = {}

    def spread_copy(key, source, target, offset):
        at = len(spreads)
        copy = pltpu.make_async_remote_copy(
            src_ref=source,
            dst_ref=target,
            send_sem=spread_send_sems.at[at],
            recv_sem=spread_recv_sems.at[at],
            device_id=peer(offset),
            device_id_type=pl.DeviceIdType.MESH,
        )
        copy.start()
        spreads.append(copy)
        spread_waits.setdefault(key, []).append(copy)

    def await_spread(key):
        for copy in spread_waits.pop(key, ()):
            copy.wait_recv()

    held = {}
    for level in (sub, top):
        plane = []
        place = jnp.int32(0)
        for step in range(row_span):
            found = [
                level_at(step * col_span + offset) == level for offset in range(col_span)
            ]
            place = jnp.where(found[0], step, place)
            plane.append(found)
        known_here = []
        for bit in range(col_bits + 1):
            here = jnp.int32(1)
            for found in plane:
                for offset in range(1 << bit):
                    here = jnp.where(found[offset], 0, here)
            known_here.append(here)
        held[level] = (place, known_here)

    def scatter_rows(source, matrix):
        for step in range(1, row_span):
            start = pl.multiple_of(flip_bits(row_at, step) * strip, strip)
            spread_copy(
                ("scatter", source),
                matrix.at[pl.ds(start, strip)],
                scattered[source].at[step],
                step * col_span,
            )
        scattered[source][0] = matrix[my_strip]

    def merged(stream, stage):
        place, known_here = held[stream_level[stream]]
        if stage == 0:
            await_spread(("scatter", SOURCES[stream]))
            return scattered[SOURCES[stream]][place]
        await_spread(("double", stream, stage - 1))
        return doubled[stream][stage - 1][known_here[stage - 1]]

    def double_cols(stream, stage):
        doubled[stream][stage][0] = merged(stream, stage)
        spread_copy(
            ("double", stream, stage),
            doubled[stream][stage].at[0],
            doubled[stream][stage].at[1],
            1 << stage if stage < col_bits else layer_size,
        )

    def gather_rows(stream, stage):
        whole[stream][my_strip] = merged(stream, stage)
        for step in range(1, row_span):
            spread_copy(
                ("gather", stream),
                whole[stream].at[my_strip],
                whole[stream].at[my_strip],
                step * col_span,
            )

    pending = [None] + [zeros for _ in range(upper_levels)]

    def scatter_up(product, slot, height):
        for level in range(1, upper_levels + 1):
            pending[level] = pending[level] + jnp.where(
                far[slot] == level + LOCAL_LEVELS - 1 - height, product, 0.0
            )

    forward = [None] * (LOCAL_COUNT + 1)
    loads[0].wait()
    loads[1].wait()
    for slot in range(2):
        forward[slot] = padded(slot, times(half(rights[slot]), lower_inverse[slot]))
    loads[2].wait()
    near = times(half(forward[0]), lower_blocks[0, 0]) + times(
        half(forward[1]), lower_blocks[1, 0]
    )
    for slot in range(2):
        scatter_up(times(half(forward[slot]), lower_blocks[slot, 1]), slot, 0)
    loads[3].wait()
    loads[4].wait()
    forward[2] = padded(2, times(half(rights[2] - near), lower_inverse[2]))
    pending[1] = pending[1] + times(half(forward[2]), lower_blocks[2, 0])
    scatter_up(times(half(forward[2]), lower_blocks[2, 1]), 2, 1)
    for level in range(1, upper_levels + 1):
        pending[level] = pending[level] - jnp.where(my_level == level, rights[OWN], 0.0)

    pl.semaphore_wait(barrier, len(partners))

    wide_columns = lax.broadcasted_iota(jnp.int32, (W, W), 1)
    wide_rows = lax.broadcasted_iota(jnp.int32, (W, W), 0)

    def own_columns(matrix):
        kept = jnp.where(
            wide_columns < widths_ref[0, OWN], matrix.astype(jnp.float32), 0.0
        )
        return half(kept)

    def own_rows(matrix):
        return jnp.where(wide_rows < widths_ref[0, OWN], matrix, 0.0)

    def lower_product(block_id):
        return jnp.dot(
            own_columns(lower_blocks[OWN, block_id]),
            lower_inverse[OWN],
            preferred_element_type=jnp.float32,
        )

    def upper_product(slot, block_id):
        return jnp.dot(
            upper_inverse[slot], upper_blocks[slot, block_id], preferred_element_type=jnp.float32
        )

    def split_times(values, matrix):
        large = half(values)
        small = half(values - large.astype(jnp.float32))
        return times(large, matrix) + times(small, matrix)

    far_is_near = jnp.full((W, W), far_ref[0, OWN], jnp.int32) == 1

    own_base = [zeros]
    residue = [None]

    def own_solve(level):
        solved = times(residue[0], fused[2])
        own_base[0] = own_base[0] + jnp.where(my_level == level, solved, 0.0)

    def far_up(level):
        product = jnp.where(my_level == level, times(residue[0], fused[1]), 0.0)
        for target in range(level + 2, upper_levels + 1):
            pending[target] = pending[target] + jnp.where(
                far[OWN] == target - level, product, 0.0
            )

    def leaf_products(slot):
        for block_id in range(NB):
            fused[3 + 2 * slot + block_id] = half(upper_product(slot, block_id))

    leaf_base = [None] * LOCAL_COUNT

    halves = {}

    def beside_up(level):
        if level == 1:
            far_product = lower_product(1)
            fused[0] = half(lower_product(0) + jnp.where(far_is_near, far_product, 0.0))
            beside_near[0] = fused[0]
            scatter_rows(0, fused.at[0])
            fused[1] = half(far_product)
            beside_far[0] = fused[1]
            loads[5].wait()
            loads[6].wait()
            fused[2] = half(
                own_rows(
                    jnp.dot(
                        own_columns(upper_inverse[OWN]),
                        lower_inverse[OWN],
                        preferred_element_type=jnp.float32,
                    )
                )
            )
            scatter_rows(1, fused.at[2])
            hand_out("beside near", fused.at[0], beside_near.at[1], col_span)
            far_product = own_rows(upper_product(OWN, 1))
            far_blocks[0] = half(far_product)
            near_blocks[0] = half(
                own_rows(upper_product(OWN, 0)) + jnp.where(far_is_near, far_product, 0.0)
            )
            fars[0] = far[OWN][: fars.shape[1], : fars.shape[2]].astype(jnp.float32)
            return
        if level < sub:
            for stream in (CHAIN, TOP_SOLVE, SUB_SOLVE):
                double_cols(stream, level - 2)
            if level == 2:
                scatter_rows(2, near_blocks.at[0])
            if level > 2:
                double_cols(BACK, level - 3)
        if level == sub - 1:
            hand_out("beside far", fused.at[1], beside_far.at[1], col_span)
            hand_out("near", near_blocks.at[0], near_blocks.at[1], 1)
        own_solve(level - 1)
        if level == sub:
            double_cols(TOP_SOLVE, col_bits)
            gather_rows(CHAIN, col_bits)
            gather_rows(SUB_SOLVE, col_bits)
            double_cols(BACK, col_bits - 1)
            await_bulk("near")
            second[0] = near_blocks[pair_place]
            hand_out("second", second.at[0], second.at[1], 2)
            hand_out("far", far_blocks.at[0], far_blocks.at[1], 1)
            hand_out("fars", fars.at[0], fars.at[1], 1)
        if level - 2 < LOCAL_COUNT:
            leaf_products(level - 2)

    near_levels = [level_at(offset) for offset in range(NEAR)]
    pair_place = jnp.where(near_levels[1] == 2, 1, 0)
    second_place = jnp.where(near_levels[2] == 2, 1, jnp.where(near_levels[3] == 2, 1, 0))

    def holder(level):
        offset_of = jnp.int32(0)
        for offset in range(2**level):
            offset_of = jnp.where(near_levels[offset] == level, offset, offset_of)
        return offset_of

    for level in range(1, sub):
        if level == sub - 1:
            for copy, at in launch([half(pending[sub]), half(pending[top])], [col_span]):
                halves["copy"], halves["at"] = copy, at
        gathered = exchange(
            [pending[level]], plans[level - 1], False, [functools.partial(beside_up, level)]
        )[0]
        residue[0] = half(-gathered)
        if level < sub - 1:
            product = times(residue[0], fused[0])
            pending[level + 1] = pending[level + 1] + jnp.where(
                my_level == level, product, 0.0
            )
            far_up(level)

    across = level_at(col_span)
    on_side = jnp.where(across == sub - 1, 1, 0)
    here = spread(jnp.where(my_level_scalar == sub - 1, 1, on_side)) == 1
    halves["copy"].wait_recv()
    await_bulk("beside near")
    await_bulk("beside far")
    products = [
        times(residue[0], beside_near[on_side]),
        times(residue[0], beside_far[on_side]),
    ]
    values = [
        pending[level]
        + incoming[halves["at"] + index].astype(jnp.float32)
        + jnp.where(here, products[index], 0.0)
        for index, level in enumerate((sub, top))
    ]
    sums = exchange(values, plans[sub - 1], False, [functools.partial(beside_up, sub)])
    gather_rows(TOP_SOLVE, col_bits + 1)
    gather_rows(BACK, col_bits)
    sub_residue = half(-sums[0])
    await_spread(("gather", CHAIN))
    layer_sum = sums[1] + times(sub_residue, whole[CHAIN][...])
    sub_base = [None]

    def beside_top():
        await_spread(("gather", SUB_SOLVE))
        sub_base[0] = times(sub_residue, whole[SUB_SOLVE][...])
        for slot in range(LOCAL_COUNT):
            leaf_base[slot] = split_times(forward[slot], upper_inverse[slot])
        await_spread(("gather", TOP_SOLVE))
        await_spread(("gather", BACK))

    total = exchange([layer_sum], plans[top - 1], False, [beside_top])[0]

    known = [None] * (upper_levels + 1)

    def pick(slot, below, lowest):
        chosen = zeros
        for level in range(lowest, upper_levels + 1):
            chosen = chosen + jnp.where(far[slot] == level - below, known[level], 0.0)
        return half(chosen)

    solved = times(half(-total), whole[TOP_SOLVE][...])
    own_solution = jnp.where(my_level == top, solved, 0.0)
    known[top] = half(solved).astype(jnp.float32)
    solved = sub_base[0] - times(half(solved), whole[BACK][...])
    own_solution = own_solution + jnp.where(my_level == sub, solved, 0.0)
    known[sub] = half(solved).astype(jnp.float32)

    for level in range(sub - 1, NEAR_BITS, -1):
        chosen = zeros
        for target in range(level + 1, upper_levels + 1):
            chosen = chosen + jnp.where(my_level + far[OWN] == target, known[target], 0.0)
        base = own_base[0] - times(half(chosen), far_blocks[0])
        solved = base - times(half(known[level + 1]), near_blocks[0])
        solved = jnp.where(my_level == level, solved, 0.0)
        own_solution = own_solution + solved

        def beside_down():
            if level == NEAR_BITS + 1:
                bases[0] = half(jnp.where(my_level == 1, own_base[0], base))
                for offset in range(1, NEAR):
                    hand_out(("base", offset), bases.at[0], bases.at[offset], offset)

        known[level] = exchange([solved], down_plans[level - 1], True, [beside_down])[0]
    for name in bulk:
        await_bulk(name)

    at = holder(1)
    reach = fars[at]
    reach = jnp.concatenate([reach] * (W // reach.shape[1]), axis=1)
    reach = jnp.concatenate([reach] * (RHS // reach.shape[0]), axis=0)
    chosen = zeros
    for target in range(3, upper_levels + 1):
        chosen = chosen + jnp.where(reach == float(target - 1), known[target], 0.0)
    base = bases[at].astype(jnp.float32) - times(half(chosen), far_blocks[at])
    solved = bases[holder(2)].astype(jnp.float32) - times(
        half(known[3]), second[second_place]
    )
    own_solution = own_solution + jnp.where(my_level == 2, solved, 0.0)
    known[2] = half(solved).astype(jnp.float32)
    solved = base - times(half(solved), near_blocks[at])
    own_solution = own_solution + jnp.where(my_level == 1, solved, 0.0)
    known[1] = half(solved).astype(jnp.float32)
    leaf_base[2] = leaf_base[2] - times(pick(2, 0, 2), fused[3 + 2 * 2 + 1])
    out_ref[0, OWN] = own_solution

    nearest = half(known[1])
    root = padded(2, leaf_base[2] - times(nearest, fused[3 + 2 * 2]))
    out_ref[0, 2] = root
    for slot in range(2):
        solved = leaf_base[slot] - times(pick(slot, -1, 1), fused[3 + 2 * slot + 1])
        solved = solved - times(half(root), fused[3 + 2 * slot])
        out_ref[0, slot] = padded(slot, solved)

    for copy, _ in sends:
        copy.wait_send()
    for copy in bulk.values():
        copy.wait_send()
    for copy in spreads:
        copy.wait_send()


def local(
    spans,
    right_sides,
    lower_inverse,
    upper_inverse,
    lower_blocks,
    upper_blocks,
    node_widths,
    far_levels,
    owner_level,
):
    layer_span, row_span, col_span = spans
    upper_levels = (layer_span * row_span * col_span).bit_length() - 1
    col_bits = col_span.bit_length() - 1
    top, sub = upper_levels, upper_levels - 1
    plans = [exchange_plan(list(range(level))) for level in range(1, sub)]
    plans.append(exchange_plan(list(range(col_bits)) + [sub - 1]))
    plans.append(exchange_plan([sub]))
    down_plans = [[]] * NEAR_BITS
    down_plans += [exchange_plan(list(range(level))) for level in range(NEAR_BITS + 1, sub)]
    vectors = [1] * (sub - 1) + [2, 1, 2] + [1] * len(down_plans)
    routes = list(zip(vectors, plans + [[[col_span]]] + down_plans))
    phases = sum(amount * len(plan) for amount, plan in routes)
    messages = sum(len(phase) for _, plan in routes for phase in plan)
    boxes = sum(amount * len(phase) for amount, plan in routes for phase in plan)
    handed = 6 + NEAR - 1
    streams, sources = len(SOURCES), len(set(SOURCES.values()))
    strip = W // row_span
    spread_count = (sources + streams) * (row_span - 1) + streams * col_bits + 1
    hbm = pl.BlockSpec(memory_space=pl.ANY)
    smem = pl.BlockSpec(memory_space=pltpu.SMEM)
    return pl.pallas_call(
        functools.partial(kernel, spans, plans, down_plans),
        out_shape=jax.ShapeDtypeStruct(right_sides.shape, jnp.float32),
        in_specs=[hbm] * 5 + [smem] * 3,
        out_specs=pl.BlockSpec(memory_space=pltpu.VMEM),
        scratch_shapes=[
            pltpu.VMEM(right_sides.shape[1:], jnp.float32),
            pltpu.VMEM(lower_inverse.shape[1:], jnp.bfloat16),
            pltpu.VMEM(upper_inverse.shape[1:], jnp.bfloat16),
            pltpu.VMEM(lower_blocks.shape[1:], jnp.bfloat16),
            pltpu.VMEM(upper_blocks.shape[1:], jnp.bfloat16),
            pltpu.VMEM((phases, RHS, W), jnp.bfloat16),
            pltpu.VMEM((boxes, RHS, W), jnp.bfloat16),
            pltpu.VMEM((3 + NB * LOCAL_COUNT, W, W), jnp.bfloat16),
            pltpu.VMEM((2, W, W), jnp.bfloat16),
            pltpu.VMEM((2, W, W), jnp.bfloat16),
            pltpu.VMEM((2, W, W), jnp.bfloat16),
            pltpu.VMEM((2, W, W), jnp.bfloat16),
            pltpu.VMEM((2, W, W), jnp.bfloat16),
            pltpu.VMEM((2, 8, 128), jnp.float32),
            pltpu.VMEM((NEAR, RHS, W), jnp.bfloat16),
            [pltpu.VMEM((row_span, strip, W), jnp.bfloat16)] * sources,
            [[pltpu.VMEM((2, strip, W), jnp.bfloat16)] * (col_bits + 1)] * streams,
            [pltpu.VMEM((W, W), jnp.bfloat16)] * streams,
            pltpu.SemaphoreType.DMA((7,)),
            pltpu.SemaphoreType.DMA((messages,)),
            pltpu.SemaphoreType.DMA((messages,)),
            pltpu.SemaphoreType.DMA((handed,)),
            pltpu.SemaphoreType.DMA((handed,)),
            pltpu.SemaphoreType.DMA((spread_count,)),
            pltpu.SemaphoreType.DMA((spread_count,)),
        ],
        compiler_params=pltpu.CompilerParams(collective_id=0, has_side_effects=True),
        name="tree_solve",
    )(
        right_sides,
        lower_inverse,
        upper_inverse,
        lower_blocks,
        upper_blocks,
        node_widths,
        far_levels,
        owner_level,
    )


def solution(mesh):
    spans = tuple(mesh.shape[axis] for axis in AXES)
    split = P(AXES)
    return jax.shard_map(
        functools.partial(local, spans),
        mesh=mesh,
        in_specs=(split,) * 7 + (P(),),
        out_specs=split,
        check_vma=False,
    )
```

```python
import functools

import jax
import jax.numpy as jnp
from jax import lax
from jax.experimental import pallas as pl
from jax.experimental.pallas import tpu as pltpu
from jax.sharding import PartitionSpec as P

W = 256
RHS = 16
NB = 2
LOCAL_LEVELS = 2
LOCAL_COUNT = 3
OWN = LOCAL_COUNT
AXES = ("gz", "row", "col")


def flip_bits(coord, mask):
    flipped = coord
    bit = 1
    while bit <= mask:
        if mask & bit:
            flipped = flipped + bit - 2 * bit * lax.rem(lax.div(coord, bit), 2)
        bit *= 2
    return flipped


def exchange_plan(bits):
    phases = []
    for low in range(0, len(bits), 4):
        offsets = [0]
        for bit in bits[low : low + 4]:
            offsets += [offset + (1 << bit) for offset in offsets]
        phases.append(offsets[:0:-1])
    return phases


def times(vectors, matrix):
    return lax.dot_general(
        vectors, matrix, (((1,), (1,)), ((), ())), preferred_element_type=jnp.float32
    )


def half(values):
    return values.astype(jnp.bfloat16)


NEAR_BITS = 2
NEAR = 2**NEAR_BITS
CHAIN, TOP_SOLVE, SUB_SOLVE, BACK = range(4)
SOURCES = {CHAIN: 0, TOP_SOLVE: 1, SUB_SOLVE: 1, BACK: 2}


def kernel(
    spans,
    plans,
    down_plans,
    rights_hbm,
    lower_inverse_hbm,
    upper_inverse_hbm,
    lower_blocks_hbm,
    upper_blocks_hbm,
    widths_ref,
    far_ref,
    owner_ref,
    out_ref,
    rights,
    lower_inverse,
    upper_inverse,
    lower_blocks,
    upper_blocks,
    outgoing,
    incoming,
    fused,
    near_blocks,
    far_blocks,
    second,
    beside_near,
    ahead,
    fars,
    bases,
    scattered,
    doubled,
    whole,
    load_sems,
    send_sems,
    recv_sems,
    bulk_send_sems,
    bulk_recv_sems,
    spread_send_sems,
    spread_recv_sems,
):
    layer_span, row_span, col_span = spans
    col_bits = col_span.bit_length() - 1
    layer_size = row_span * col_span
    upper_levels = len(plans)
    top, sub = upper_levels, upper_levels - 1
    layer_at = lax.axis_index("gz")
    row_at = lax.axis_index("row")
    col_at = lax.axis_index("col")
    device = (layer_at * row_span + row_at) * col_span + col_at

    def peer(offset):
        return (
            flip_bits(layer_at, offset // layer_size),
            flip_bits(row_at, offset // col_span % row_span),
            flip_bits(col_at, offset % col_span),
        )

    pieces = [
        (rights_hbm.at[0], rights),
        (lower_inverse_hbm.at[0, pl.ds(0, 2)], lower_inverse.at[pl.ds(0, 2)]),
        (lower_blocks_hbm.at[0, pl.ds(0, 2)], lower_blocks.at[pl.ds(0, 2)]),
        (lower_inverse_hbm.at[0, pl.ds(2, 2)], lower_inverse.at[pl.ds(2, 2)]),
        (lower_blocks_hbm.at[0, pl.ds(2, 2)], lower_blocks.at[pl.ds(2, 2)]),
        (upper_blocks_hbm.at[0], upper_blocks),
        (upper_inverse_hbm.at[0], upper_inverse),
    ]
    loads = [
        pltpu.make_async_copy(source, target, load_sems.at[at])
        for at, (source, target) in enumerate(pieces)
    ]
    for load in loads:
        load.start()

    barrier = pltpu.get_barrier_semaphore()
    partners = {offset for plan in plans + down_plans for phase in plan for offset in phase}
    partners = sorted(partners | {step * col_span for step in range(1, row_span)})
    for offset in partners:
        pl.semaphore_signal(
            barrier, inc=1, device_id=peer(offset), device_id_type=pl.DeviceIdType.MESH
        )

    columns = lax.broadcasted_iota(jnp.int32, (RHS, W), 1)

    def spread(scalar):
        return jnp.full((RHS, W), scalar, jnp.int32)

    inside = [columns < widths_ref[0, slot] for slot in range(LOCAL_COUNT + 1)]
    far = [spread(far_ref[0, slot]) for slot in range(LOCAL_COUNT + 1)]
    my_level_scalar = owner_ref[device]
    my_level = spread(my_level_scalar)
    zeros = jnp.zeros((RHS, W), jnp.float32)

    steps = []
    for bit in range(upper_levels):
        size = 1 << bit
        steps.append(size - 2 * size * lax.rem(lax.div(device, size), 2))

    def level_at(offset):
        at = device
        for bit in range(upper_levels):
            if offset >> bit & 1:
                at = at + steps[bit]
        return owner_ref[at]

    def padded(slot, values):
        return jnp.where(inside[slot], values, 0.0)

    counts = [0, 0, 0]
    sends = []

    def launch(rounded, phase):
        outbox, amount = counts[0], len(rounded)
        counts[0] += amount
        for index, part in enumerate(rounded):
            outgoing[outbox + index] = part
        copies = []
        for offset in phase:
            at, message = counts[1], counts[2]
            counts[1] += amount
            counts[2] += 1
            copy = pltpu.make_async_remote_copy(
                src_ref=outgoing.at[pl.ds(outbox, amount)],
                dst_ref=incoming.at[pl.ds(at, amount)],
                send_sem=send_sems.at[message],
                recv_sem=recv_sems.at[message],
                device_id=peer(offset),
                device_id_type=pl.DeviceIdType.MESH,
            )
            copy.start()
            copies.append((copy, at))
        sends.extend(copies)
        return copies

    bulk = {}

    def hand_out(name, source, target, offset):
        at = len(bulk)
        bulk[name] = pltpu.make_async_remote_copy(
            src_ref=source,
            dst_ref=target,
            send_sem=bulk_send_sems.at[at],
            recv_sem=bulk_recv_sems.at[at],
            device_id=peer(offset),
            device_id_type=pl.DeviceIdType.MESH,
        )
        bulk[name].start()

    received = set()

    def await_bulk(name):
        if name not in received:
            received.add(name)
            bulk[name].wait_recv()

    def exchange(values, plan, narrow, besides, started=None):
        for index, phase in enumerate(plan):
            rounded = [half(value) for value in values]
            copies = started if started and index == 0 else launch(rounded, phase)
            if index < len(besides):
                besides[index]()
            if narrow:
                values = [part.astype(jnp.float32) for part in rounded]
            for copy, at in copies:
                copy.wait_recv()
                values = [
                    value + incoming[at + part].astype(jnp.float32)
                    for part, value in enumerate(values)
                ]
        return values

    strip = W // row_span
    my_strip = pl.ds(pl.multiple_of(row_at * strip, strip), strip)
    stream_level = {CHAIN: sub, TOP_SOLVE: top, SUB_SOLVE: sub, BACK: sub}
    spreads = []
    spread_waits = {}

    def spread_copy(key, source, target, offset):
        at = len(spreads)
        copy = pltpu.make_async_remote_copy(
            src_ref=source,
            dst_ref=target,
            send_sem=spread_send_sems.at[at],
            recv_sem=spread_recv_sems.at[at],
            device_id=peer(offset),
            device_id_type=pl.DeviceIdType.MESH,
        )
        copy.start()
        spreads.append(copy)
        spread_waits.setdefault(key, []).append(copy)

    def await_spread(key):
        for copy in spread_waits.pop(key, ()):
            copy.wait_recv()

    held = {}
    for level in (sub, top):
        place = jnp.int32(0)
        known_here = []
        here = jnp.int32(1)
        layers = (0,) if level == sub else (0, layer_size)
        rounds = [(0, 1)] + [(1 << bit, 2 << bit) for bit in range(col_bits)]
        for layer in layers:
            for low, high in rounds if layer == layers[-1] else rounds[:1]:
                for others in layers if low else (layer,):
                    for step in range(row_span):
                        for offset in range(low, high):
                            found = level_at(others + step * col_span + offset) == level
                            here = jnp.where(found, 0, here)
                            if layer == others == low == 0:
                                place = jnp.where(found, step, place)
                known_here.append(here)
        held[level] = (place, known_here)

    def reach_of(stream, stage):
        if stream == TOP_SOLVE:
            return 1 << stage - 1 if stage else layer_size
        return 1 << stage

    def scatter_rows(source, matrix):
        for step in range(1, row_span):
            start = pl.multiple_of(flip_bits(row_at, step) * strip, strip)
            spread_copy(
                ("scatter", source),
                matrix.at[pl.ds(start, strip)],
                scattered[source].at[step],
                step * col_span,
            )
        scattered[source][0] = matrix[my_strip]

    def merged(stream, stage):
        place, known_here = held[stream_level[stream]]
        if stage == 0:
            await_spread(("scatter", SOURCES[stream]))
            return scattered[SOURCES[stream]][place]
        await_spread(("double", stream, stage - 1))
        return doubled[stream][stage - 1][known_here[stage - 1]]

    def double_cols(stream, stage):
        doubled[stream][stage][0] = merged(stream, stage)
        spread_copy(
            ("double", stream, stage),
            doubled[stream][stage].at[0],
            doubled[stream][stage].at[1],
            reach_of(stream, stage),
        )

    def gather_rows(stream, stage):
        whole[stream][my_strip] = merged(stream, stage)
        for step in range(1, row_span):
            spread_copy(
                ("gather", stream),
                whole[stream].at[my_strip],
                whole[stream].at[my_strip],
                step * col_span,
            )

    pending = [None] + [zeros for _ in range(upper_levels)]

    def scatter_up(product, slot, height):
        for level in range(1, upper_levels + 1):
            pending[level] = pending[level] + jnp.where(
                far[slot] == level + LOCAL_LEVELS - 1 - height, product, 0.0
            )

    forward = [None] * (LOCAL_COUNT + 1)
    loads[0].wait()
    loads[1].wait()
    for slot in range(2):
        forward[slot] = padded(slot, times(half(rights[slot]), lower_inverse[slot]))
    loads[2].wait()
    near = times(half(forward[0]), lower_blocks[0, 0]) + times(
        half(forward[1]), lower_blocks[1, 0]
    )
    for slot in range(2):
        scatter_up(times(half(forward[slot]), lower_blocks[slot, 1]), slot, 0)
    loads[3].wait()
    loads[4].wait()
    forward[2] = padded(2, times(half(rights[2] - near), lower_inverse[2]))
    pending[1] = pending[1] + times(half(forward[2]), lower_blocks[2, 0])
    scatter_up(times(half(forward[2]), lower_blocks[2, 1]), 2, 1)
    for level in range(1, upper_levels + 1):
        pending[level] = pending[level] - jnp.where(my_level == level, rights[OWN], 0.0)

    wide_columns = lax.broadcasted_iota(jnp.int32, (W, W), 1)
    wide_rows = lax.broadcasted_iota(jnp.int32, (W, W), 0)

    def own_columns(matrix):
        kept = jnp.where(
            wide_columns < widths_ref[0, OWN], matrix.astype(jnp.float32), 0.0
        )
        return half(kept)

    def own_rows(matrix):
        return jnp.where(wide_rows < widths_ref[0, OWN], matrix, 0.0)

    def lower_product(block_id):
        return jnp.dot(
            own_columns(lower_blocks[OWN, block_id]),
            lower_inverse[OWN],
            preferred_element_type=jnp.float32,
        )

    def upper_product(slot, block_id):
        return jnp.dot(
            upper_inverse[slot], upper_blocks[slot, block_id], preferred_element_type=jnp.float32
        )

    def split_times(values, matrix):
        large = half(values)
        small = half(values - large.astype(jnp.float32))
        return times(large, matrix) + times(small, matrix)

    far_is_near = jnp.full((W, W), far_ref[0, OWN], jnp.int32) == 1

    far_product = lower_product(1)
    fused[0] = half(lower_product(0) + jnp.where(far_is_near, far_product, 0.0))
    beside_near[0] = fused[0]
    fused[1] = half(far_product)
    loads[5].wait()
    loads[6].wait()
    fused[2] = half(
        own_rows(
            jnp.dot(
                own_columns(upper_inverse[OWN]),
                lower_inverse[OWN],
                preferred_element_type=jnp.float32,
            )
        )
    )
    far_product = own_rows(upper_product(OWN, 1))
    far_blocks[0] = half(far_product)
    near_blocks[0] = half(
        own_rows(upper_product(OWN, 0)) + jnp.where(far_is_near, far_product, 0.0)
    )
    ahead[0] = near_blocks[0]
    fars[0] = far[OWN][: fars.shape[1], : fars.shape[2]].astype(jnp.float32)

    pl.semaphore_wait(barrier, len(partners))

    own_base = [zeros]
    residue = [None]

    def own_solve(level):
        solved = times(residue[0], fused[2])
        own_base[0] = own_base[0] + jnp.where(my_level == level, solved, 0.0)

    def far_up(level):
        product = jnp.where(my_level == level, times(residue[0], fused[1]), 0.0)
        for target in range(level + 2, upper_levels + 1):
            pending[target] = pending[target] + jnp.where(
                far[OWN] == target - level, product, 0.0
            )

    def leaf_products(slot):
        for block_id in range(NB):
            fused[3 + 2 * slot + block_id] = half(upper_product(slot, block_id))

    leaf_base = [None] * LOCAL_COUNT

    def first_round():
        scatter_rows(0, fused.at[0])
        scatter_rows(1, fused.at[2])
        scatter_rows(2, near_blocks.at[0])
        hand_ahead(0)
        hand_out("near", near_blocks.at[0], near_blocks.at[1], 1)

    near_levels = [level_at(offset) for offset in range(NEAR)]
    halves = {}

    def hand_ahead(part):
        rows = pl.ds(part * (W // 2), W // 2)
        hand_out(("ahead", part), near_blocks.at[0, rows], ahead.at[1, rows], 2)

    def hand_beside(part):
        rows = pl.ds(part * (W // 2), W // 2)
        hand_out(
            ("beside", part), fused.at[0, rows], beside_near.at[1, rows], col_span
        )

    def beside_up(level):
        if level == 1:
            first_round()
            return
        if level == 2:
            hand_ahead(1)
        if level == sub - 1:
            hand_beside(1)
        if level < sub:
            if level > 2:
                double_cols(BACK, level - 3)
            double_cols(CHAIN, level - 2)
            if level == 2:
                double_cols(TOP_SOLVE, 0)
            double_cols(SUB_SOLVE, level - 2)
            if level == 2:
                hand_beside(0)
            double_cols(TOP_SOLVE, level - 1)
            if level == sub - 1:
                double_cols(BACK, level - 2)
        own_solve(level - 1)
        if level == sub:
            gather_rows(CHAIN, col_bits)
            gather_rows(SUB_SOLVE, col_bits)
            gather_rows(TOP_SOLVE, col_bits + 1)
            gather_rows(BACK, col_bits)
            await_bulk(("ahead", 0))
            await_bulk(("ahead", 1))
            second[0] = ahead[ahead_place]
            hand_out("second", second.at[0], second.at[1], 1)
            hand_out("far", far_blocks.at[0], far_blocks.at[1], 1)
            hand_out("fars", fars.at[0], fars.at[1], 1)
        if level - 2 < LOCAL_COUNT:
            leaf_products(level - 2)

    ahead_place = jnp.where(near_levels[2] == 2, 1, 0)
    second_place = jnp.where(near_levels[1] == 2, 1, jnp.where(near_levels[3] == 2, 1, 0))

    def holder(level):
        offset_of = jnp.int32(0)
        for offset in range(2**level):
            offset_of = jnp.where(near_levels[offset] == level, offset, offset_of)
        return offset_of

    for level in range(1, sub):
        if level == sub - 1:
            for copy, at in launch([half(pending[sub])], [col_span]):
                halves["copy"], halves["at"] = copy, at
        gathered = exchange(
            [pending[level]], plans[level - 1], False, [functools.partial(beside_up, level)]
        )[0]
        residue[0] = half(-gathered)
        if level < sub - 1:
            product = times(residue[0], fused[0])
            pending[level + 1] = pending[level + 1] + jnp.where(
                my_level == level, product, 0.0
            )
            far_up(level)

    across = level_at(col_span)
    on_side = jnp.where(across == sub - 1, 1, 0)
    here = spread(jnp.where(my_level_scalar == sub - 1, 1, on_side)) == 1
    halves["copy"].wait_recv()
    far_up(sub - 1)
    await_bulk(("beside", 0))
    await_bulk(("beside", 1))
    product = times(residue[0], beside_near[on_side])
    value = (
        pending[sub]
        + incoming[halves["at"]].astype(jnp.float32)
        + jnp.where(here, product, 0.0)
    )
    layer_plan = down_plans[-1]

    def beside_sub():
        halves["layer"] = launch([half(pending[top])], layer_plan[0])
        beside_up(sub)

    sums = exchange([value], plans[sub - 1], False, [beside_sub])
    sub_residue = half(-sums[0])
    await_spread(("gather", CHAIN))
    chained = times(sub_residue, whole[CHAIN][...])
    layer_sum = exchange([pending[top]], layer_plan, False, [], halves["layer"])[0] + chained
    sub_base = [None]

    def beside_top():
        await_spread(("gather", SUB_SOLVE))
        sub_base[0] = times(sub_residue, whole[SUB_SOLVE][...])
        for slot in range(LOCAL_COUNT):
            leaf_base[slot] = split_times(forward[slot], upper_inverse[slot])
        await_spread(("gather", TOP_SOLVE))
        await_spread(("gather", BACK))

    total = exchange([layer_sum], plans[top - 1], False, [beside_top])[0]

    known = [None] * (upper_levels + 1)

    def pick(slot, below, lowest):
        chosen = zeros
        for level in range(lowest, upper_levels + 1):
            chosen = chosen + jnp.where(far[slot] == level - below, known[level], 0.0)
        return half(chosen)

    solved = times(half(-total), whole[TOP_SOLVE][...])
    own_solution = jnp.where(my_level == top, solved, 0.0)
    known[top] = half(solved).astype(jnp.float32)
    solved = sub_base[0] - times(half(solved), whole[BACK][...])
    own_solution = own_solution + jnp.where(my_level == sub, solved, 0.0)
    known[sub] = half(solved).astype(jnp.float32)

    for level in range(sub - 1, NEAR_BITS, -1):
        chosen = zeros
        for target in range(level + 1, upper_levels + 1):
            chosen = chosen + jnp.where(my_level + far[OWN] == target, known[target], 0.0)
        base = own_base[0] - times(half(chosen), far_blocks[0])
        solved = base - times(half(known[level + 1]), near_blocks[0])
        solved = jnp.where(my_level == level, solved, 0.0)
        own_solution = own_solution + solved

        def beside_down():
            if level == NEAR_BITS + 1:
                bases[0] = half(jnp.where(my_level == 1, own_base[0], base))
                for offset in range(1, NEAR):
                    hand_out(("base", offset), bases.at[0], bases.at[offset], offset)

        known[level] = exchange([solved], down_plans[level - 1], True, [beside_down])[0]
    for name in bulk:
        await_bulk(name)

    at = holder(1)
    reach = fars[at]
    reach = jnp.concatenate([reach] * (W // reach.shape[1]), axis=1)
    reach = jnp.concatenate([reach] * (RHS // reach.shape[0]), axis=0)
    chosen = zeros
    for target in range(3, upper_levels + 1):
        chosen = chosen + jnp.where(reach == float(target - 1), known[target], 0.0)
    base = bases[at].astype(jnp.float32) - times(half(chosen), far_blocks[at])
    solved = bases[holder(2)].astype(jnp.float32) - times(
        half(known[3]), second[second_place]
    )
    own_solution = own_solution + jnp.where(my_level == 2, solved, 0.0)
    known[2] = half(solved).astype(jnp.float32)
    solved = base - times(half(solved), near_blocks[at])
    own_solution = own_solution + jnp.where(my_level == 1, solved, 0.0)
    known[1] = half(solved).astype(jnp.float32)
    leaf_base[2] = leaf_base[2] - times(pick(2, 0, 2), fused[3 + 2 * 2 + 1])
    out_ref[0, OWN] = own_solution

    nearest = half(known[1])
    root = padded(2, leaf_base[2] - times(nearest, fused[3 + 2 * 2]))
    out_ref[0, 2] = root
    for slot in range(2):
        solved = leaf_base[slot] - times(pick(slot, -1, 1), fused[3 + 2 * slot + 1])
        solved = solved - times(half(root), fused[3 + 2 * slot])
        out_ref[0, slot] = padded(slot, solved)

    for copy, _ in sends:
        copy.wait_send()
    for copy in bulk.values():
        copy.wait_send()
    for copy in spreads:
        copy.wait_send()


def local(
    spans,
    right_sides,
    lower_inverse,
    upper_inverse,
    lower_blocks,
    upper_blocks,
    node_widths,
    far_levels,
    owner_level,
):
    layer_span, row_span, col_span = spans
    upper_levels = (layer_span * row_span * col_span).bit_length() - 1
    col_bits = col_span.bit_length() - 1
    top, sub = upper_levels, upper_levels - 1
    plans = [exchange_plan(list(range(level))) for level in range(1, sub)]
    plans.append(exchange_plan(list(range(col_bits)) + [sub - 1]))
    plans.append(exchange_plan([sub]))
    down_plans = [[]] * NEAR_BITS
    down_plans += [exchange_plan(list(range(level))) for level in range(NEAR_BITS + 1, sub)]
    down_plans.append(exchange_plan(list(range(sub))))
    vectors = [1] * (sub + 2 + len(down_plans))
    routes = list(zip(vectors, plans + [[[col_span]]] + down_plans))
    phases = sum(amount * len(plan) for amount, plan in routes)
    messages = sum(len(phase) for _, plan in routes for phase in plan)
    boxes = sum(amount * len(phase) for amount, plan in routes for phase in plan)
    handed = 8 + NEAR - 1
    streams, sources = len(SOURCES), len(set(SOURCES.values()))
    strip = W // row_span
    spread_count = (sources + streams) * (row_span - 1) + streams * col_bits + 1
    hbm = pl.BlockSpec(memory_space=pl.ANY)
    smem = pl.BlockSpec(memory_space=pltpu.SMEM)
    return pl.pallas_call(
        functools.partial(kernel, spans, plans, down_plans),
        out_shape=jax.ShapeDtypeStruct(right_sides.shape, jnp.float32),
        in_specs=[hbm] * 5 + [smem] * 3,
        out_specs=pl.BlockSpec(memory_space=pltpu.VMEM),
        scratch_shapes=[
            pltpu.VMEM(right_sides.shape[1:], jnp.float32),
            pltpu.VMEM(lower_inverse.shape[1:], jnp.bfloat16),
            pltpu.VMEM(upper_inverse.shape[1:], jnp.bfloat16),
            pltpu.VMEM(lower_blocks.shape[1:], jnp.bfloat16),
            pltpu.VMEM(upper_blocks.shape[1:], jnp.bfloat16),
            pltpu.VMEM((phases, RHS, W), jnp.bfloat16),
            pltpu.VMEM((boxes, RHS, W), jnp.bfloat16),
            pltpu.VMEM((3 + NB * LOCAL_COUNT, W, W), jnp.bfloat16),
            pltpu.VMEM((2, W, W), jnp.bfloat16),
            pltpu.VMEM((2, W, W), jnp.bfloat16),
            pltpu.VMEM((2, W, W), jnp.bfloat16),
            pltpu.VMEM((2, W, W), jnp.bfloat16),
            pltpu.VMEM((2, W, W), jnp.bfloat16),
            pltpu.VMEM((2, 8, 128), jnp.float32),
            pltpu.VMEM((NEAR, RHS, W), jnp.bfloat16),
            [pltpu.VMEM((row_span, strip, W), jnp.bfloat16)] * sources,
            [[pltpu.VMEM((2, strip, W), jnp.bfloat16)] * (col_bits + 1)] * streams,
            [pltpu.VMEM((W, W), jnp.bfloat16)] * streams,
            pltpu.SemaphoreType.DMA((7,)),
            pltpu.SemaphoreType.DMA((messages,)),
            pltpu.SemaphoreType.DMA((messages,)),
            pltpu.SemaphoreType.DMA((handed,)),
            pltpu.SemaphoreType.DMA((handed,)),
            pltpu.SemaphoreType.DMA((spread_count,)),
            pltpu.SemaphoreType.DMA((spread_count,)),
        ],
        compiler_params=pltpu.CompilerParams(collective_id=0, has_side_effects=True),
        name="tree_solve",
    )(
        right_sides,
        lower_inverse,
        upper_inverse,
        lower_blocks,
        upper_blocks,
        node_widths,
        far_levels,
        owner_level,
    )


def solution(mesh):
    spans = tuple(mesh.shape[axis] for axis in AXES)
    split = P(AXES)
    return jax.shard_map(
        functools.partial(local, spans),
        mesh=mesh,
        in_specs=(split,) * 7 + (P(),),
        out_specs=split,
        check_vma=False,
    )
```

```python
import functools

import jax
import jax.numpy as jnp
from jax import lax
from jax.experimental import pallas as pl
from jax.experimental.pallas import tpu as pltpu
from jax.sharding import PartitionSpec as P

W = 256
RHS = 16
NB = 2
LOCAL_LEVELS = 2
LOCAL_COUNT = 3
OWN = LOCAL_COUNT
AXES = ("gz", "row", "col")


def flip_bits(coord, mask):
    flipped = coord
    bit = 1
    while bit <= mask:
        if mask & bit:
            flipped = flipped + bit - 2 * bit * lax.rem(lax.div(coord, bit), 2)
        bit *= 2
    return flipped


def exchange_plan(bits):
    phases = []
    for low in range(0, len(bits), 4):
        offsets = [0]
        for bit in bits[low : low + 4]:
            offsets += [offset + (1 << bit) for offset in offsets]
        phases.append(offsets[:0:-1])
    return phases


def times(vectors, matrix):
    return lax.dot_general(
        vectors, matrix, (((1,), (1,)), ((), ())), preferred_element_type=jnp.float32
    )


def half(values):
    return values.astype(jnp.bfloat16)


NEAR_BITS = 2
NEAR = 2**NEAR_BITS
CHAIN, TOP_SOLVE, SUB_SOLVE, BACK = range(4)
SOURCES = {CHAIN: 0, TOP_SOLVE: 1, SUB_SOLVE: 1, BACK: 2}


def kernel(
    spans,
    plans,
    down_plans,
    rights_hbm,
    lower_inverse_hbm,
    upper_inverse_hbm,
    lower_blocks_hbm,
    upper_blocks_hbm,
    widths_ref,
    far_ref,
    owner_ref,
    out_hbm,
    rights,
    lower_inverse,
    upper_inverse,
    lower_blocks,
    upper_blocks,
    outgoing,
    incoming,
    fused,
    near_blocks,
    far_blocks,
    second,
    beside_near,
    ahead,
    fars,
    bases,
    scattered,
    doubled,
    whole,
    solved_slots,
    load_sems,
    store_sems,
    send_sems,
    recv_sems,
    bulk_send_sems,
    bulk_recv_sems,
    spread_send_sems,
    spread_recv_sems,
):
    layer_span, row_span, col_span = spans
    col_bits = col_span.bit_length() - 1
    layer_size = row_span * col_span
    upper_levels = len(plans)
    top, sub = upper_levels, upper_levels - 1
    layer_at = lax.axis_index("gz")
    row_at = lax.axis_index("row")
    col_at = lax.axis_index("col")
    device = (layer_at * row_span + row_at) * col_span + col_at

    def peer(offset):
        return (
            flip_bits(layer_at, offset // layer_size),
            flip_bits(row_at, offset // col_span % row_span),
            flip_bits(col_at, offset % col_span),
        )

    pieces = [
        (rights_hbm.at[0], rights),
        (lower_inverse_hbm.at[0, pl.ds(0, 2)], lower_inverse.at[pl.ds(0, 2)]),
        (lower_blocks_hbm.at[0, pl.ds(0, 2)], lower_blocks.at[pl.ds(0, 2)]),
        (lower_inverse_hbm.at[0, pl.ds(2, 2)], lower_inverse.at[pl.ds(2, 2)]),
        (lower_blocks_hbm.at[0, pl.ds(2, 2)], lower_blocks.at[pl.ds(2, 2)]),
        (upper_blocks_hbm.at[0], upper_blocks),
        (upper_inverse_hbm.at[0], upper_inverse),
    ]
    loads = [
        pltpu.make_async_copy(source, target, load_sems.at[at])
        for at, (source, target) in enumerate(pieces)
    ]
    for load in loads:
        load.start()

    barrier = pltpu.get_barrier_semaphore()
    partners = {offset for plan in plans + down_plans for phase in plan for offset in phase}
    partners = sorted(partners | {step * col_span for step in range(1, row_span)})
    for offset in partners:
        pl.semaphore_signal(
            barrier, inc=1, device_id=peer(offset), device_id_type=pl.DeviceIdType.MESH
        )

    columns = lax.broadcasted_iota(jnp.int32, (RHS, W), 1)

    def spread(scalar):
        return jnp.full((RHS, W), scalar, jnp.int32)

    inside = [columns < widths_ref[0, slot] for slot in range(LOCAL_COUNT + 1)]
    far = [spread(far_ref[0, slot]) for slot in range(LOCAL_COUNT + 1)]
    my_level_scalar = owner_ref[device]
    my_level = spread(my_level_scalar)
    zeros = jnp.zeros((RHS, W), jnp.float32)

    steps = []
    for bit in range(upper_levels):
        size = 1 << bit
        steps.append(size - 2 * size * lax.rem(lax.div(device, size), 2))

    def level_at(offset):
        at = device
        for bit in range(upper_levels):
            if offset >> bit & 1:
                at = at + steps[bit]
        return owner_ref[at]

    def padded(slot, values):
        return jnp.where(inside[slot], values, 0.0)

    counts = [0, 0, 0]
    sends = []

    class Joined:
        def __init__(self, target, send_sem, recv_sem):
            self.sent = pltpu.make_async_copy(target, target, send_sem)
            self.arrived = pltpu.make_async_copy(target, target, recv_sem)

        def wait_recv(self):
            self.arrived.wait()

        def wait_send(self):
            self.sent.wait()

    def launch(rounded, phase):
        outbox, amount = counts[0], len(rounded)
        counts[0] += amount
        for index, part in enumerate(rounded):
            outgoing[outbox + index] = part
        begin, message = counts[1], counts[2]
        counts[1] += amount * len(phase)
        counts[2] += 1
        for index, offset in enumerate(phase):
            pltpu.make_async_remote_copy(
                src_ref=outgoing.at[pl.ds(outbox, amount)],
                dst_ref=incoming.at[pl.ds(begin + index * amount, amount)],
                send_sem=send_sems.at[message],
                recv_sem=recv_sems.at[message],
                device_id=peer(offset),
                device_id_type=pl.DeviceIdType.MESH,
            ).start()
        copy = Joined(
            incoming.at[pl.ds(begin, amount * len(phase))],
            send_sems.at[message],
            recv_sems.at[message],
        )
        copies = [(copy, begin + index * amount) for index in range(len(phase))]
        sends.append(copies[0])
        return copies

    bulk = {}
    drained = set()
    spreads = []

    def drain():
        copies = [copy for copy, _ in sends] + list(bulk.values()) + spreads
        for copy in copies:
            if id(copy) not in drained:
                drained.add(id(copy))
                copy.wait_send()

    stores = []

    def store_out(slots):
        store = pltpu.make_async_copy(
            solved_slots.at[slots], out_hbm.at[0, slots], store_sems.at[len(stores)]
        )
        store.start()
        stores.append(store)

    def hand_out(name, source, target, offset):
        at = len(bulk)
        bulk[name] = pltpu.make_async_remote_copy(
            src_ref=source,
            dst_ref=target,
            send_sem=bulk_send_sems.at[at],
            recv_sem=bulk_recv_sems.at[at],
            device_id=peer(offset),
            device_id_type=pl.DeviceIdType.MESH,
        )
        bulk[name].start()

    received = set()

    def await_bulk(name):
        if name not in received:
            received.add(name)
            bulk[name].wait_recv()

    def exchange(values, plan, narrow, besides, started=None):
        for index, phase in enumerate(plan):
            rounded = [half(value) for value in values]
            copies = started if started and index == 0 else launch(rounded, phase)
            if index < len(besides):
                besides[index]()
            if narrow:
                values = [part.astype(jnp.float32) for part in rounded]
            copies[0][0].wait_recv()
            for _, at in copies:
                values = [
                    value + incoming[at + part].astype(jnp.float32)
                    for part, value in enumerate(values)
                ]
        return values

    strip = W // row_span
    my_strip = pl.ds(pl.multiple_of(row_at * strip, strip), strip)
    stream_level = {CHAIN: sub, TOP_SOLVE: top, SUB_SOLVE: sub, BACK: sub}
    spread_waits = {}

    def spread_copies(key, pairs, extent):
        at = len(spreads)
        for source, target, offset in pairs:
            pltpu.make_async_remote_copy(
                src_ref=source,
                dst_ref=target,
                send_sem=spread_send_sems.at[at],
                recv_sem=spread_recv_sems.at[at],
                device_id=peer(offset),
                device_id_type=pl.DeviceIdType.MESH,
            ).start()
        copy = Joined(extent, spread_send_sems.at[at], spread_recv_sems.at[at])
        spreads.append(copy)
        spread_waits[key] = [copy]

    def await_spread(key):
        for copy in spread_waits.pop(key, ()):
            copy.wait_recv()

    held = {}
    for level in (sub, top):
        place = jnp.int32(0)
        known_here = []
        here = jnp.int32(1)
        layers = (0,) if level == sub else (0, layer_size)
        rounds = [(0, 1)] + [(1 << bit, 2 << bit) for bit in range(col_bits)]
        for layer in layers:
            for low, high in rounds if layer == layers[-1] else rounds[:1]:
                for others in layers if low else (layer,):
                    for step in range(row_span):
                        for offset in range(low, high):
                            found = level_at(others + step * col_span + offset) == level
                            here = jnp.where(found, 0, here)
                            if layer == others == low == 0:
                                place = jnp.where(found, step, place)
                known_here.append(here)
        held[level] = (place, known_here)

    def reach_of(stream, stage):
        if stream == TOP_SOLVE:
            return 1 << stage - 1 if stage else layer_size
        return 1 << stage

    others = pl.ds(1, row_span - 1)

    def scatter_rows(source, matrix):
        pairs = []
        for step in range(1, row_span):
            start = pl.multiple_of(flip_bits(row_at, step) * strip, strip)
            rows = matrix.at[pl.ds(start, strip)]
            pairs.append((rows, scattered[source].at[step], step * col_span))
        spread_copies(("scatter", source), pairs, scattered[source].at[others])
        scattered[source][0] = matrix[my_strip]

    def merged(stream, stage):
        place, known_here = held[stream_level[stream]]
        if stage == 0:
            await_spread(("scatter", SOURCES[stream]))
            return scattered[SOURCES[stream]][place]
        await_spread(("double", stream, stage - 1))
        return doubled[stream][stage - 1][known_here[stage - 1]]

    def double_cols(stream, stage):
        mine, theirs = (doubled[stream][stage].at[side] for side in range(2))
        doubled[stream][stage][0] = merged(stream, stage)
        pairs = [(mine, theirs, reach_of(stream, stage))]
        spread_copies(("double", stream, stage), pairs, theirs)

    def gather_rows(stream, stage):
        whole[stream][my_strip] = merged(stream, stage)
        rows = whole[stream].at[my_strip]
        pairs = [(rows, rows, step * col_span) for step in range(1, row_span)]
        extent = whole[stream].at[pl.ds(0, strip * (row_span - 1))]
        spread_copies(("gather", stream), pairs, extent)

    pending = [None] + [zeros for _ in range(upper_levels)]

    def scatter_up(product, slot, height):
        for level in range(1, upper_levels + 1):
            pending[level] = pending[level] + jnp.where(
                far[slot] == level + LOCAL_LEVELS - 1 - height, product, 0.0
            )

    forward = [None] * (LOCAL_COUNT + 1)
    loads[0].wait()
    loads[1].wait()
    for slot in range(2):
        forward[slot] = padded(slot, times(half(rights[slot]), lower_inverse[slot]))
    loads[2].wait()
    near = times(half(forward[0]), lower_blocks[0, 0]) + times(
        half(forward[1]), lower_blocks[1, 0]
    )
    for slot in range(2):
        scatter_up(times(half(forward[slot]), lower_blocks[slot, 1]), slot, 0)
    loads[3].wait()
    loads[4].wait()
    forward[2] = padded(2, times(half(rights[2] - near), lower_inverse[2]))
    pending[1] = pending[1] + times(half(forward[2]), lower_blocks[2, 0])
    scatter_up(times(half(forward[2]), lower_blocks[2, 1]), 2, 1)
    for level in range(1, upper_levels + 1):
        pending[level] = pending[level] - jnp.where(my_level == level, rights[OWN], 0.0)

    wide_columns = lax.broadcasted_iota(jnp.int32, (W, W), 1)
    wide_rows = lax.broadcasted_iota(jnp.int32, (W, W), 0)

    def own_columns(matrix):
        kept = jnp.where(
            wide_columns < widths_ref[0, OWN], matrix.astype(jnp.float32), 0.0
        )
        return half(kept)

    def own_rows(matrix):
        return jnp.where(wide_rows < widths_ref[0, OWN], matrix, 0.0)

    def lower_product(block_id):
        return jnp.dot(
            own_columns(lower_blocks[OWN, block_id]),
            lower_inverse[OWN],
            preferred_element_type=jnp.float32,
        )

    def upper_product(slot, block_id):
        return jnp.dot(
            upper_inverse[slot], upper_blocks[slot, block_id], preferred_element_type=jnp.float32
        )

    def split_times(values, matrix):
        large = half(values)
        small = half(values - large.astype(jnp.float32))
        return times(large, matrix) + times(small, matrix)

    far_is_near = jnp.full((W, W), far_ref[0, OWN], jnp.int32) == 1

    far_product = lower_product(1)
    fused[0] = half(lower_product(0) + jnp.where(far_is_near, far_product, 0.0))
    beside_near[0] = fused[0]
    fused[1] = half(far_product)
    loads[5].wait()
    loads[6].wait()
    fused[2] = half(
        own_rows(
            jnp.dot(
                own_columns(upper_inverse[OWN]),
                lower_inverse[OWN],
                preferred_element_type=jnp.float32,
            )
        )
    )
    far_product = own_rows(upper_product(OWN, 1))
    far_blocks[0] = half(far_product)
    near_blocks[0] = half(
        own_rows(upper_product(OWN, 0)) + jnp.where(far_is_near, far_product, 0.0)
    )
    ahead[0] = near_blocks[0]
    fars[0] = far[OWN][: fars.shape[1], : fars.shape[2]].astype(jnp.float32)

    pl.semaphore_wait(barrier, len(partners))

    own_base = [zeros]
    residue = [None]

    def own_solve(level):
        solved = times(residue[0], fused[2])
        own_base[0] = own_base[0] + jnp.where(my_level == level, solved, 0.0)

    def far_up(level):
        product = jnp.where(my_level == level, times(residue[0], fused[1]), 0.0)
        for target in range(level + 2, upper_levels + 1):
            pending[target] = pending[target] + jnp.where(
                far[OWN] == target - level, product, 0.0
            )

    def leaf_products(slot):
        for block_id in range(NB):
            fused[3 + 2 * slot + block_id] = half(upper_product(slot, block_id))
        if slot == 2:
            kept = half(
                jnp.where(
                    wide_rows < widths_ref[0, 2], fused[3 + 2 * 2].astype(jnp.float32), 0.0
                )
            )
            for leaf in range(2):
                fused[9 + leaf] = half(
                    jnp.dot(
                        fused[3 + 2 * leaf], kept, preferred_element_type=jnp.float32
                    )
                )

    leaf_base = [None] * LOCAL_COUNT

    def first_round():
        scatter_rows(0, fused.at[0])
        scatter_rows(1, fused.at[2])
        scatter_rows(2, near_blocks.at[0])
        hand_ahead(0)
        hand_out("near", near_blocks.at[0], near_blocks.at[1], 1)

    near_levels = [level_at(offset) for offset in range(NEAR)]
    halves = {}

    def hand_ahead(part):
        rows = pl.ds(part * (W // 2), W // 2)
        hand_out(("ahead", part), near_blocks.at[0, rows], ahead.at[1, rows], 2)

    def hand_beside(part):
        rows = pl.ds(part * (W // 2), W // 2)
        hand_out(
            ("beside", part), fused.at[0, rows], beside_near.at[1, rows], col_span
        )

    def beside_up(level):
        if level == 1:
            first_round()
            return
        if level == 2:
            hand_ahead(1)
        if level == sub - 1:
            hand_beside(1)
        if level < sub:
            if level > 2:
                double_cols(BACK, level - 3)
            double_cols(CHAIN, level - 2)
            if level == 2:
                double_cols(TOP_SOLVE, 0)
            double_cols(SUB_SOLVE, level - 2)
            if level == 2:
                hand_beside(0)
            double_cols(TOP_SOLVE, level - 1)
            if level == sub - 1:
                double_cols(BACK, level - 2)
        own_solve(level - 1)
        if level == sub:
            gather_rows(CHAIN, col_bits)
            gather_rows(SUB_SOLVE, col_bits)
            gather_rows(TOP_SOLVE, col_bits + 1)
            gather_rows(BACK, col_bits)
            await_bulk(("ahead", 0))
            await_bulk(("ahead", 1))
            second[0] = ahead[ahead_place]
            hand_out("second", second.at[0], second.at[1], 1)
            hand_out("far", far_blocks.at[0], far_blocks.at[1], 1)
            hand_out("fars", fars.at[0], fars.at[1], 1)
        if level - 2 < LOCAL_COUNT:
            leaf_products(level - 2)

    ahead_place = jnp.where(near_levels[2] == 2, 1, 0)
    second_place = jnp.where(near_levels[1] == 2, 1, jnp.where(near_levels[3] == 2, 1, 0))

    def holder(level):
        offset_of = jnp.int32(0)
        for offset in range(2**level):
            offset_of = jnp.where(near_levels[offset] == level, offset, offset_of)
        return offset_of

    for level in range(1, sub):
        if level == sub - 1:
            for copy, at in launch([half(pending[sub])], [col_span]):
                halves["copy"], halves["at"] = copy, at
        gathered = exchange(
            [pending[level]], plans[level - 1], False, [functools.partial(beside_up, level)]
        )[0]
        residue[0] = half(-gathered)
        if level < sub - 1:
            product = times(residue[0], fused[0])
            pending[level + 1] = pending[level + 1] + jnp.where(
                my_level == level, product, 0.0
            )
            far_up(level)

    across = level_at(col_span)
    on_side = jnp.where(across == sub - 1, 1, 0)
    here = spread(jnp.where(my_level_scalar == sub - 1, 1, on_side)) == 1
    halves["copy"].wait_recv()
    far_up(sub - 1)
    await_bulk(("beside", 0))
    await_bulk(("beside", 1))
    product = times(residue[0], beside_near[on_side])
    value = (
        pending[sub]
        + incoming[halves["at"]].astype(jnp.float32)
        + jnp.where(here, product, 0.0)
    )
    layer_plan = down_plans[-1]

    def beside_sub():
        halves["layer"] = launch([half(pending[top])], layer_plan[0])
        beside_up(sub)

    sums = exchange([value], plans[sub - 1], False, [beside_sub])
    sub_residue = half(-sums[0])
    await_spread(("gather", CHAIN))
    chained = times(sub_residue, whole[CHAIN][...])
    layer_sum = exchange([pending[top]], layer_plan, False, [], halves["layer"])[0] + chained
    sub_base = [None]

    def beside_top():
        await_spread(("gather", SUB_SOLVE))
        sub_base[0] = times(sub_residue, whole[SUB_SOLVE][...])
        for slot in range(LOCAL_COUNT):
            leaf_base[slot] = split_times(forward[slot], upper_inverse[slot])
        await_spread(("gather", TOP_SOLVE))
        await_spread(("gather", BACK))

    total = exchange([layer_sum], plans[top - 1], False, [beside_top])[0]

    known = [None] * (upper_levels + 1)

    def pick(slot, below, lowest):
        chosen = zeros
        for level in range(lowest, upper_levels + 1):
            chosen = chosen + jnp.where(far[slot] == level - below, known[level], 0.0)
        return half(chosen)

    solved = times(half(-total), whole[TOP_SOLVE][...])
    own_solution = jnp.where(my_level == top, solved, 0.0)
    known[top] = half(solved).astype(jnp.float32)
    solved = sub_base[0] - times(half(solved), whole[BACK][...])
    own_solution = own_solution + jnp.where(my_level == sub, solved, 0.0)
    known[sub] = half(solved).astype(jnp.float32)

    marks = [len(sends), len(bulk), len(spreads)]
    for level in range(sub - 1, NEAR_BITS, -1):
        chosen = zeros
        for target in range(level + 1, upper_levels + 1):
            chosen = chosen + jnp.where(my_level + far[OWN] == target, known[target], 0.0)
        base = own_base[0] - times(half(chosen), far_blocks[0])
        solved = base - times(half(known[level + 1]), near_blocks[0])
        solved = jnp.where(my_level == level, solved, 0.0)
        own_solution = own_solution + solved

        def beside_down():
            if level == NEAR_BITS + 1:
                bases[0] = half(jnp.where(my_level == 1, own_base[0], base))
                for offset in range(1, NEAR):
                    hand_out(("base", offset), bases.at[0], bases.at[offset], offset)
                for name in bulk:
                    if name[0] != "base":
                        await_bulk(name)
            copies = [copy for copy, _ in sends[: marks[0]]]
            copies += list(bulk.values())[: marks[1]] + spreads[: marks[2]]
            for copy in copies:
                if id(copy) not in drained:
                    drained.add(id(copy))
                    copy.wait_send()

        known[level] = exchange([solved], down_plans[level - 1], True, [beside_down])[0]
    for name in bulk:
        await_bulk(name)

    at = holder(1)
    reach = fars[at]
    reach = jnp.concatenate([reach] * (W // reach.shape[1]), axis=1)
    reach = jnp.concatenate([reach] * (RHS // reach.shape[0]), axis=0)
    chosen = zeros
    for target in range(3, upper_levels + 1):
        chosen = chosen + jnp.where(reach == float(target - 1), known[target], 0.0)
    base = bases[at].astype(jnp.float32) - times(half(chosen), far_blocks[at])
    solved = bases[holder(2)].astype(jnp.float32) - times(
        half(known[3]), second[second_place]
    )
    own_solution = own_solution + jnp.where(my_level == 2, solved, 0.0)
    known[2] = half(solved).astype(jnp.float32)
    solved = base - times(half(solved), near_blocks[at])
    own_solution = own_solution + jnp.where(my_level == 1, solved, 0.0)
    known[1] = half(solved).astype(jnp.float32)
    solved_slots[OWN] = own_solution
    store_out(pl.ds(OWN, 1))
    nearest = half(known[1])
    root_base = leaf_base[2] - times(pick(2, 0, 2), fused[3 + 2 * 2 + 1])
    solved_slots[2] = padded(2, root_base - times(nearest, fused[3 + 2 * 2]))
    store_out(pl.ds(2, 1))
    root_part = half(padded(2, root_base))
    for slot in range(2):
        solved = leaf_base[slot] - times(pick(slot, -1, 1), fused[3 + 2 * slot + 1])
        solved = solved - times(root_part, fused[3 + 2 * slot])
        solved_slots[slot] = padded(slot, solved + times(nearest, fused[9 + slot]))

    store_out(pl.ds(0, 2))
    drain()
    for store in stores:
        store.wait()


def local(
    spans,
    right_sides,
    lower_inverse,
    upper_inverse,
    lower_blocks,
    upper_blocks,
    node_widths,
    far_levels,
    owner_level,
):
    layer_span, row_span, col_span = spans
    upper_levels = (layer_span * row_span * col_span).bit_length() - 1
    col_bits = col_span.bit_length() - 1
    top, sub = upper_levels, upper_levels - 1
    plans = [exchange_plan(list(range(level))) for level in range(1, sub)]
    plans.append(exchange_plan(list(range(col_bits)) + [sub - 1]))
    plans.append(exchange_plan([sub]))
    down_plans = [[]] * NEAR_BITS
    down_plans += [exchange_plan(list(range(level))) for level in range(NEAR_BITS + 1, sub)]
    down_plans.append(exchange_plan(list(range(sub))))
    vectors = [1] * (sub + 2 + len(down_plans))
    routes = list(zip(vectors, plans + [[[col_span]]] + down_plans))
    phases = sum(amount * len(plan) for amount, plan in routes)
    messages = sum(len(plan) for _, plan in routes)
    boxes = sum(amount * len(phase) for amount, plan in routes for phase in plan)
    handed = 8 + NEAR - 1
    streams, sources = len(SOURCES), len(set(SOURCES.values()))
    strip = W // row_span
    spread_count = sources + streams * (col_bits + 1) + 1
    hbm = pl.BlockSpec(memory_space=pl.ANY)
    smem = pl.BlockSpec(memory_space=pltpu.SMEM)
    return pl.pallas_call(
        functools.partial(kernel, spans, plans, down_plans),
        out_shape=jax.ShapeDtypeStruct(right_sides.shape, jnp.float32),
        in_specs=[hbm] * 5 + [smem] * 3,
        out_specs=hbm,
        scratch_shapes=[
            pltpu.VMEM(right_sides.shape[1:], jnp.float32),
            pltpu.VMEM(lower_inverse.shape[1:], jnp.bfloat16),
            pltpu.VMEM(upper_inverse.shape[1:], jnp.bfloat16),
            pltpu.VMEM(lower_blocks.shape[1:], jnp.bfloat16),
            pltpu.VMEM(upper_blocks.shape[1:], jnp.bfloat16),
            pltpu.VMEM((phases, RHS, W), jnp.bfloat16),
            pltpu.VMEM((boxes, RHS, W), jnp.bfloat16),
            pltpu.VMEM((5 + NB * LOCAL_COUNT, W, W), jnp.bfloat16),
            pltpu.VMEM((2, W, W), jnp.bfloat16),
            pltpu.VMEM((2, W, W), jnp.bfloat16),
            pltpu.VMEM((2, W, W), jnp.bfloat16),
            pltpu.VMEM((2, W, W), jnp.bfloat16),
            pltpu.VMEM((2, W, W), jnp.bfloat16),
            pltpu.VMEM((2, 8, 128), jnp.float32),
            pltpu.VMEM((NEAR, RHS, W), jnp.bfloat16),
            [pltpu.VMEM((row_span, strip, W), jnp.bfloat16)] * sources,
            [[pltpu.VMEM((2, strip, W), jnp.bfloat16)] * (col_bits + 1)] * streams,
            [pltpu.VMEM((W, W), jnp.bfloat16)] * streams,
            pltpu.VMEM(right_sides.shape[1:], jnp.float32),
            pltpu.SemaphoreType.DMA((7,)),
            pltpu.SemaphoreType.DMA((3,)),
            pltpu.SemaphoreType.DMA((messages,)),
            pltpu.SemaphoreType.DMA((messages,)),
            pltpu.SemaphoreType.DMA((handed,)),
            pltpu.SemaphoreType.DMA((handed,)),
            pltpu.SemaphoreType.DMA((spread_count,)),
            pltpu.SemaphoreType.DMA((spread_count,)),
        ],
        compiler_params=pltpu.CompilerParams(collective_id=0, has_side_effects=True),
        name="tree_solve",
    )(
        right_sides,
        lower_inverse,
        upper_inverse,
        lower_blocks,
        upper_blocks,
        node_widths,
        far_levels,
        owner_level,
    )


def solution(mesh):
    spans = tuple(mesh.shape[axis] for axis in AXES)
    split = P(AXES)
    return jax.shard_map(
        functools.partial(local, spans),
        mesh=mesh,
        in_specs=(split,) * 7 + (P(),),
        out_specs=split,
        check_vma=False,
    )
```

```python
import functools

import jax
import jax.numpy as jnp
from jax import lax
from jax.experimental import pallas as pl
from jax.experimental.pallas import tpu as pltpu
from jax.sharding import PartitionSpec as P

W = 256
RHS = 16
NB = 2
LOCAL_LEVELS = 2
LOCAL_COUNT = 3
OWN = LOCAL_COUNT
AXES = ("gz", "row", "col")


def flip_bits(coord, mask):
    flipped = coord
    bit = 1
    while bit <= mask:
        if mask & bit:
            flipped = flipped + bit - 2 * bit * lax.rem(lax.div(coord, bit), 2)
        bit *= 2
    return flipped


def exchange_plan(bits):
    phases = []
    for low in range(0, len(bits), 4):
        offsets = [0]
        for bit in bits[low : low + 4]:
            offsets += [offset + (1 << bit) for offset in offsets]
        phases.append(offsets[:0:-1])
    return phases


def times(vectors, matrix):
    return lax.dot_general(
        vectors, matrix, (((1,), (1,)), ((), ())), preferred_element_type=jnp.float32
    )


def half(values):
    return values.astype(jnp.bfloat16)


NEAR_BITS = 2
NEAR = 2**NEAR_BITS
CHAIN, TOP_SOLVE, SUB_SOLVE, BACK = range(4)
SOURCES = {CHAIN: 0, TOP_SOLVE: 1, SUB_SOLVE: 1, BACK: 2}


def kernel(
    spans,
    plans,
    down_plans,
    rights_hbm,
    lower_inverse_hbm,
    upper_inverse_hbm,
    lower_blocks_hbm,
    upper_blocks_hbm,
    widths_ref,
    far_ref,
    owner_ref,
    out_hbm,
    rights,
    lower_inverse,
    upper_inverse,
    lower_blocks,
    upper_blocks,
    outgoing,
    incoming,
    fused,
    near_blocks,
    far_blocks,
    second,
    beside_near,
    ahead,
    fars,
    bases,
    scattered,
    doubled,
    whole,
    solved_slots,
    sent_strips,
    load_sems,
    store_sems,
    send_sems,
    recv_sems,
    bulk_send_sems,
    bulk_recv_sems,
    spread_send_sems,
    spread_recv_sems,
):
    layer_span, row_span, col_span = spans
    col_bits = col_span.bit_length() - 1
    layer_size = row_span * col_span
    upper_levels = len(plans)
    top, sub = upper_levels, upper_levels - 1
    layer_at = lax.axis_index("gz")
    row_at = lax.axis_index("row")
    col_at = lax.axis_index("col")
    device = (layer_at * row_span + row_at) * col_span + col_at

    def peer(offset):
        return (
            flip_bits(layer_at, offset // layer_size),
            flip_bits(row_at, offset // col_span % row_span),
            flip_bits(col_at, offset % col_span),
        )

    pieces = [
        (rights_hbm.at[0], rights),
        (lower_inverse_hbm.at[0], lower_inverse),
        (lower_blocks_hbm.at[0], lower_blocks),
        (upper_blocks_hbm.at[0], upper_blocks),
        (upper_inverse_hbm.at[0], upper_inverse),
    ]
    loads = [
        pltpu.make_async_copy(source, target, load_sems.at[at])
        for at, (source, target) in enumerate(pieces)
    ]
    for load in loads:
        load.start()

    barrier = pltpu.get_barrier_semaphore()
    partners = {offset for plan in plans + down_plans for phase in plan for offset in phase}
    partners = sorted(partners | {step * col_span for step in range(1, row_span)})
    for offset in partners:
        pl.semaphore_signal(
            barrier, inc=1, device_id=peer(offset), device_id_type=pl.DeviceIdType.MESH
        )

    columns = lax.broadcasted_iota(jnp.int32, (RHS, W), 1)

    def spread(scalar):
        return jnp.full((RHS, W), scalar, jnp.int32)

    inside = [columns < widths_ref[0, slot] for slot in range(LOCAL_COUNT + 1)]
    far = [spread(far_ref[0, slot]) for slot in range(LOCAL_COUNT + 1)]
    my_level_scalar = owner_ref[device]
    my_level = spread(my_level_scalar)
    zeros = jnp.zeros((RHS, W), jnp.float32)

    steps = []
    for bit in range(upper_levels):
        size = 1 << bit
        steps.append(size - 2 * size * lax.rem(lax.div(device, size), 2))

    def level_at(offset):
        at = device
        for bit in range(upper_levels):
            if offset >> bit & 1:
                at = at + steps[bit]
        return owner_ref[at]

    def padded(slot, values):
        return jnp.where(inside[slot], values, 0.0)

    counts = [0, 0, 0]
    sends = []

    class Joined:
        def __init__(self, target, send_sem, recv_sem):
            self.sent = pltpu.make_async_copy(target, target, send_sem)
            self.arrived = pltpu.make_async_copy(target, target, recv_sem)

        def wait_recv(self):
            self.arrived.wait()

        def wait_send(self):
            self.sent.wait()

    def launch(rounded, phase):
        outbox, amount = counts[0], len(rounded)
        counts[0] += amount
        for index, part in enumerate(rounded):
            outgoing[outbox + index] = part
        begin, message = counts[1], counts[2]
        counts[1] += amount * len(phase)
        counts[2] += 1
        for index, offset in enumerate(phase):
            pltpu.make_async_remote_copy(
                src_ref=outgoing.at[pl.ds(outbox, amount)],
                dst_ref=incoming.at[pl.ds(begin + index * amount, amount)],
                send_sem=send_sems.at[0],
                recv_sem=recv_sems.at[message],
                device_id=peer(offset),
                device_id_type=pl.DeviceIdType.MESH,
            ).start()
        copy = Joined(
            incoming.at[pl.ds(begin, amount * len(phase))],
            send_sems.at[0],
            recv_sems.at[message],
        )
        copies = [(copy, begin + index * amount) for index in range(len(phase))]
        sends.append(copies[0])
        return copies

    bulk = {}
    spreads = []
    strips_sent = [0]
    vectors_sent = [0]

    def drain():
        for copy in bulk.values():
            copy.wait_send()
        pltpu.make_async_copy(incoming, incoming, send_sems.at[0]).wait()
        pltpu.make_async_copy(sent_strips, sent_strips, spread_send_sems.at[0]).wait()

    stores = []

    def store_out(slots):
        store = pltpu.make_async_copy(
            solved_slots.at[slots], out_hbm.at[0, slots], store_sems.at[len(stores)]
        )
        store.start()
        stores.append(store)

    def hand_out(name, source, target, offset):
        at = len(bulk)
        bulk[name] = pltpu.make_async_remote_copy(
            src_ref=source,
            dst_ref=target,
            send_sem=bulk_send_sems.at[at],
            recv_sem=bulk_recv_sems.at[at],
            device_id=peer(offset),
            device_id_type=pl.DeviceIdType.MESH,
        )
        bulk[name].start()

    received = set()

    def await_bulk(name):
        if name not in received:
            received.add(name)
            bulk[name].wait_recv()

    def exchange(values, plan, narrow, besides, started=None):
        for index, phase in enumerate(plan):
            rounded = [half(value) for value in values]
            copies = started if started and index == 0 else launch(rounded, phase)
            if index < len(besides):
                besides[index]()
            if narrow:
                values = [part.astype(jnp.float32) for part in rounded]
            copies[0][0].wait_recv()
            for _, at in copies:
                values = [
                    value + incoming[at + part].astype(jnp.float32)
                    for part, value in enumerate(values)
                ]
        return values

    strip = W // row_span
    my_strip = pl.ds(pl.multiple_of(row_at * strip, strip), strip)
    stream_level = {CHAIN: sub, TOP_SOLVE: top, SUB_SOLVE: sub, BACK: sub}
    spread_waits = {}

    def spread_copies(key, pairs, extent):
        at = len(spreads)
        for source, target, offset in pairs:
            pltpu.make_async_remote_copy(
                src_ref=source,
                dst_ref=target,
                send_sem=spread_send_sems.at[0],
                recv_sem=spread_recv_sems.at[at],
                device_id=peer(offset),
                device_id_type=pl.DeviceIdType.MESH,
            ).start()
        strips_sent[0] += len(pairs)
        copy = Joined(extent, spread_send_sems.at[0], spread_recv_sems.at[at])
        spreads.append(copy)
        spread_waits[key] = [copy]

    def await_spread(key):
        for copy in spread_waits.pop(key, ()):
            copy.wait_recv()

    held = {}
    for level in (sub, top):
        place = jnp.int32(0)
        known_here = []
        here = jnp.int32(1)
        layers = (0,) if level == sub else (0, layer_size)
        rounds = [(0, 1)] + [(1 << bit, 2 << bit) for bit in range(col_bits)]
        for layer in layers:
            for low, high in rounds if layer == layers[-1] else rounds[:1]:
                for others in layers if low else (layer,):
                    for step in range(row_span):
                        for offset in range(low, high):
                            found = level_at(others + step * col_span + offset) == level
                            here = jnp.where(found, 0, here)
                            if layer == others == low == 0:
                                place = jnp.where(found, step, place)
                known_here.append(here)
        held[level] = (place, known_here)

    def reach_of(stream, stage):
        if stream == TOP_SOLVE:
            return 1 << stage - 1 if stage else layer_size
        return 1 << stage

    others = pl.ds(1, row_span - 1)

    def scatter_rows(source, matrix):
        pairs = []
        for step in range(1, row_span):
            start = pl.multiple_of(flip_bits(row_at, step) * strip, strip)
            rows = matrix.at[pl.ds(start, strip)]
            pairs.append((rows, scattered[source].at[step], step * col_span))
        spread_copies(("scatter", source), pairs, scattered[source].at[others])
        scattered[source][0] = matrix[my_strip]

    def merged(stream, stage):
        place, known_here = held[stream_level[stream]]
        if stage == 0:
            await_spread(("scatter", SOURCES[stream]))
            return scattered[SOURCES[stream]][place]
        await_spread(("double", stream, stage - 1))
        return doubled[stream][stage - 1][known_here[stage - 1]]

    def double_cols(stream, stage):
        mine, theirs = (doubled[stream][stage].at[side] for side in range(2))
        doubled[stream][stage][0] = merged(stream, stage)
        pairs = [(mine, theirs, reach_of(stream, stage))]
        spread_copies(("double", stream, stage), pairs, theirs)

    def gather_rows(stream, stage):
        whole[stream][my_strip] = merged(stream, stage)
        rows = whole[stream].at[my_strip]
        pairs = [(rows, rows, step * col_span) for step in range(1, row_span)]
        extent = whole[stream].at[pl.ds(0, strip * (row_span - 1))]
        spread_copies(("gather", stream), pairs, extent)

    pending = [None] + [zeros for _ in range(upper_levels)]

    def scatter_up(product, slot, height):
        for level in range(1, upper_levels + 1):
            pending[level] = pending[level] + jnp.where(
                far[slot] == level + LOCAL_LEVELS - 1 - height, product, 0.0
            )

    forward = [None] * (LOCAL_COUNT + 1)
    loads[0].wait()
    loads[1].wait()
    for slot in range(2):
        forward[slot] = padded(slot, times(half(rights[slot]), lower_inverse[slot]))
    loads[2].wait()
    near = times(half(forward[0]), lower_blocks[0, 0]) + times(
        half(forward[1]), lower_blocks[1, 0]
    )
    for slot in range(2):
        scatter_up(times(half(forward[slot]), lower_blocks[slot, 1]), slot, 0)
    forward[2] = padded(2, times(half(rights[2] - near), lower_inverse[2]))
    pending[1] = pending[1] + times(half(forward[2]), lower_blocks[2, 0])
    scatter_up(times(half(forward[2]), lower_blocks[2, 1]), 2, 1)
    for level in range(1, upper_levels + 1):
        pending[level] = pending[level] - jnp.where(my_level == level, rights[OWN], 0.0)

    wide_columns = lax.broadcasted_iota(jnp.int32, (W, W), 1)
    wide_rows = lax.broadcasted_iota(jnp.int32, (W, W), 0)

    def own_columns(matrix):
        kept = jnp.where(
            wide_columns < widths_ref[0, OWN], matrix.astype(jnp.float32), 0.0
        )
        return half(kept)

    def own_rows(matrix):
        return jnp.where(wide_rows < widths_ref[0, OWN], matrix, 0.0)

    def lower_product(block_id):
        return jnp.dot(
            own_columns(lower_blocks[OWN, block_id]),
            lower_inverse[OWN],
            preferred_element_type=jnp.float32,
        )

    def upper_product(slot, block_id):
        return jnp.dot(
            upper_inverse[slot], upper_blocks[slot, block_id], preferred_element_type=jnp.float32
        )

    def split_times(values, matrix):
        large = half(values)
        small = half(values - large.astype(jnp.float32))
        return times(large, matrix) + times(small, matrix)

    far_is_near = jnp.full((W, W), far_ref[0, OWN], jnp.int32) == 1

    far_product = lower_product(1)
    fused[0] = half(lower_product(0) + jnp.where(far_is_near, far_product, 0.0))
    beside_near[0] = fused[0]
    fused[1] = half(far_product)
    loads[3].wait()
    loads[4].wait()
    fused[2] = half(
        own_rows(
            jnp.dot(
                own_columns(upper_inverse[OWN]),
                lower_inverse[OWN],
                preferred_element_type=jnp.float32,
            )
        )
    )
    far_product = own_rows(upper_product(OWN, 1))
    far_blocks[0] = half(far_product)
    near_blocks[0] = half(
        own_rows(upper_product(OWN, 0)) + jnp.where(far_is_near, far_product, 0.0)
    )
    ahead[0] = near_blocks[0]
    fars[0] = far[OWN][: fars.shape[1], : fars.shape[2]].astype(jnp.float32)

    pl.semaphore_wait(barrier, len(partners))

    own_base = [zeros]
    residue = [None]

    def own_solve(level):
        solved = times(residue[0], fused[2])
        own_base[0] = own_base[0] + jnp.where(my_level == level, solved, 0.0)

    def far_up(level):
        product = jnp.where(my_level == level, times(residue[0], fused[1]), 0.0)
        for target in range(level + 2, upper_levels + 1):
            pending[target] = pending[target] + jnp.where(
                far[OWN] == target - level, product, 0.0
            )

    def leaf_products(slot):
        for block_id in range(NB):
            fused[3 + 2 * slot + block_id] = half(upper_product(slot, block_id))
        if slot == 2:
            kept = half(
                jnp.where(
                    wide_rows < widths_ref[0, 2], fused[3 + 2 * 2].astype(jnp.float32), 0.0
                )
            )
            for leaf in range(2):
                fused[9 + leaf] = half(
                    jnp.dot(
                        fused[3 + 2 * leaf], kept, preferred_element_type=jnp.float32
                    )
                )

    leaf_base = [None] * LOCAL_COUNT

    def first_round():
        scatter_rows(0, fused.at[0])
        scatter_rows(1, fused.at[2])
        scatter_rows(2, near_blocks.at[0])
        hand_ahead(0)
        hand_out("near", near_blocks.at[0], near_blocks.at[1], 1)

    near_levels = [level_at(offset) for offset in range(NEAR)]
    halves = {}

    def hand_ahead(part):
        rows = pl.ds(part * (W // 2), W // 2)
        hand_out(("ahead", part), near_blocks.at[0, rows], ahead.at[1, rows], 2)

    def hand_beside(part):
        rows = pl.ds(part * (W // 2), W // 2)
        hand_out(
            ("beside", part), fused.at[0, rows], beside_near.at[1, rows], col_span
        )

    def beside_up(level):
        if level == 1:
            first_round()
            return
        if level == 2:
            hand_ahead(1)
        if level == sub - 1:
            hand_beside(1)
        if level < sub:
            double_cols(CHAIN, level - 2)
            if level > 2:
                double_cols(BACK, level - 3)
            if level == 2:
                double_cols(TOP_SOLVE, 0)
            double_cols(SUB_SOLVE, level - 2)
            if level == 2:
                hand_beside(0)
            double_cols(TOP_SOLVE, level - 1)
            if level == sub - 1:
                double_cols(BACK, level - 2)
        own_solve(level - 1)
        if level == sub:
            gather_rows(CHAIN, col_bits)
            gather_rows(SUB_SOLVE, col_bits)
            gather_rows(TOP_SOLVE, col_bits + 1)
            gather_rows(BACK, col_bits)
            await_bulk(("ahead", 0))
            await_bulk(("ahead", 1))
            second[0] = ahead[ahead_place]
            hand_out("second", second.at[0], second.at[1], 1)
            hand_out("far", far_blocks.at[0], far_blocks.at[1], 1)
            hand_out("fars", fars.at[0], fars.at[1], 1)
        if level - 2 < LOCAL_COUNT:
            leaf_products(level - 2)

    ahead_place = jnp.where(near_levels[2] == 2, 1, 0)
    second_place = jnp.where(near_levels[1] == 2, 1, jnp.where(near_levels[3] == 2, 1, 0))

    def holder(level):
        offset_of = jnp.int32(0)
        for offset in range(2**level):
            offset_of = jnp.where(near_levels[offset] == level, offset, offset_of)
        return offset_of

    for level in range(1, sub):
        if level == sub - 1:
            for copy, at in launch([half(pending[sub])], [col_span]):
                halves["copy"], halves["at"] = copy, at
        gathered = exchange(
            [pending[level]], plans[level - 1], False, [functools.partial(beside_up, level)]
        )[0]
        residue[0] = half(-gathered)
        if level < sub - 1:
            product = times(residue[0], fused[0])
            pending[level + 1] = pending[level + 1] + jnp.where(
                my_level == level, product, 0.0
            )
            far_up(level)

    across = level_at(col_span)
    on_side = jnp.where(across == sub - 1, 1, 0)
    here = spread(jnp.where(my_level_scalar == sub - 1, 1, on_side)) == 1
    halves["copy"].wait_recv()
    far_up(sub - 1)
    await_bulk(("beside", 0))
    await_bulk(("beside", 1))
    product = times(residue[0], beside_near[on_side])
    value = (
        pending[sub]
        + incoming[halves["at"]].astype(jnp.float32)
        + jnp.where(here, product, 0.0)
    )
    layer_plan = down_plans[-1]

    def beside_sub():
        halves["layer"] = launch([half(pending[top])], layer_plan[0])
        beside_up(sub)

    sums = exchange([value], plans[sub - 1], False, [beside_sub])
    sub_residue = half(-sums[0])
    await_spread(("gather", CHAIN))
    chained = times(sub_residue, whole[CHAIN][...])
    layer_sum = exchange([pending[top]], layer_plan, False, [], halves["layer"])[0] + chained
    sub_base = [None]

    def beside_top():
        await_spread(("gather", SUB_SOLVE))
        sub_base[0] = times(sub_residue, whole[SUB_SOLVE][...])
        for slot in range(LOCAL_COUNT):
            leaf_base[slot] = split_times(forward[slot], upper_inverse[slot])
        await_spread(("gather", TOP_SOLVE))
        await_spread(("gather", BACK))

    total = exchange([layer_sum], plans[top - 1], False, [beside_top])[0]

    known = [None] * (upper_levels + 1)

    def pick(slot, below, lowest):
        chosen = zeros
        for level in range(lowest, upper_levels + 1):
            chosen = chosen + jnp.where(far[slot] == level - below, known[level], 0.0)
        return half(chosen)

    solved = times(half(-total), whole[TOP_SOLVE][...])
    own_solution = jnp.where(my_level == top, solved, 0.0)
    known[top] = half(solved).astype(jnp.float32)
    solved = sub_base[0] - times(half(solved), whole[BACK][...])
    own_solution = own_solution + jnp.where(my_level == sub, solved, 0.0)
    known[sub] = half(solved).astype(jnp.float32)

    for level in range(sub - 1, NEAR_BITS, -1):
        chosen = zeros
        for target in range(level + 1, upper_levels + 1):
            chosen = chosen + jnp.where(my_level + far[OWN] == target, known[target], 0.0)
        base = own_base[0] - times(half(chosen), far_blocks[0])
        solved = base - times(half(known[level + 1]), near_blocks[0])
        solved = jnp.where(my_level == level, solved, 0.0)
        own_solution = own_solution + solved

        def beside_down():
            if level == NEAR_BITS + 1:
                bases[0] = half(jnp.where(my_level == 1, own_base[0], base))
                for offset in range(1, NEAR):
                    hand_out(("base", offset), bases.at[0], bases.at[offset], offset)
                for name in bulk:
                    if name[0] != "base":
                        await_bulk(name)

        known[level] = exchange([solved], down_plans[level - 1], True, [beside_down])[0]
    for name in bulk:
        await_bulk(name)

    at = holder(1)
    reach = fars[at]
    reach = jnp.concatenate([reach] * (W // reach.shape[1]), axis=1)
    reach = jnp.concatenate([reach] * (RHS // reach.shape[0]), axis=0)
    chosen = zeros
    for target in range(3, upper_levels + 1):
        chosen = chosen + jnp.where(reach == float(target - 1), known[target], 0.0)
    base = bases[at].astype(jnp.float32) - times(half(chosen), far_blocks[at])
    solved = bases[holder(2)].astype(jnp.float32) - times(
        half(known[3]), second[second_place]
    )
    own_solution = own_solution + jnp.where(my_level == 2, solved, 0.0)
    known[2] = half(solved).astype(jnp.float32)
    solved = base - times(half(solved), near_blocks[at])
    own_solution = own_solution + jnp.where(my_level == 1, solved, 0.0)
    known[1] = half(solved).astype(jnp.float32)
    solved_slots[OWN] = own_solution
    store_out(pl.ds(OWN, 1))
    nearest = half(known[1])
    root_base = leaf_base[2] - times(pick(2, 0, 2), fused[3 + 2 * 2 + 1])
    solved_slots[2] = padded(2, root_base - times(nearest, fused[3 + 2 * 2]))
    root_part = half(padded(2, root_base))
    for slot in range(2):
        solved = leaf_base[slot] - times(pick(slot, -1, 1), fused[3 + 2 * slot + 1])
        solved = solved - times(root_part, fused[3 + 2 * slot])
        solved_slots[slot] = padded(slot, solved + times(nearest, fused[9 + slot]))

    store_out(pl.ds(0, 3))
    drain()
    for store in stores:
        store.wait()


def local(
    spans,
    right_sides,
    lower_inverse,
    upper_inverse,
    lower_blocks,
    upper_blocks,
    node_widths,
    far_levels,
    owner_level,
):
    layer_span, row_span, col_span = spans
    upper_levels = (layer_span * row_span * col_span).bit_length() - 1
    col_bits = col_span.bit_length() - 1
    top, sub = upper_levels, upper_levels - 1
    plans = [exchange_plan(list(range(level))) for level in range(1, sub)]
    plans.append(exchange_plan(list(range(col_bits)) + [sub - 1]))
    plans.append(exchange_plan([sub]))
    down_plans = [[]] * NEAR_BITS
    down_plans += [exchange_plan(list(range(level))) for level in range(NEAR_BITS + 1, sub)]
    down_plans.append(exchange_plan(list(range(sub))))
    vectors = [1] * (sub + 2 + len(down_plans))
    routes = list(zip(vectors, plans + [[[col_span]]] + down_plans))
    phases = sum(amount * len(plan) for amount, plan in routes)
    messages = sum(len(plan) for _, plan in routes)
    boxes = sum(amount * len(phase) for amount, plan in routes for phase in plan)
    handed = 8 + NEAR - 1
    streams, sources = len(SOURCES), len(set(SOURCES.values()))
    strip = W // row_span
    strips = (sources + streams) * (row_span - 1) + streams * col_bits + 1
    spread_count = sources + streams * (col_bits + 1) + 1
    hbm = pl.BlockSpec(memory_space=pl.ANY)
    smem = pl.BlockSpec(memory_space=pltpu.SMEM)
    return pl.pallas_call(
        functools.partial(kernel, spans, plans, down_plans),
        out_shape=jax.ShapeDtypeStruct(right_sides.shape, jnp.float32),
        in_specs=[hbm] * 5 + [smem] * 3,
        out_specs=hbm,
        scratch_shapes=[
            pltpu.VMEM(right_sides.shape[1:], jnp.float32),
            pltpu.VMEM(lower_inverse.shape[1:], jnp.bfloat16),
            pltpu.VMEM(upper_inverse.shape[1:], jnp.bfloat16),
            pltpu.VMEM(lower_blocks.shape[1:], jnp.bfloat16),
            pltpu.VMEM(upper_blocks.shape[1:], jnp.bfloat16),
            pltpu.VMEM((phases, RHS, W), jnp.bfloat16),
            pltpu.VMEM((boxes, RHS, W), jnp.bfloat16),
            pltpu.VMEM((5 + NB * LOCAL_COUNT, W, W), jnp.bfloat16),
            pltpu.VMEM((2, W, W), jnp.bfloat16),
            pltpu.VMEM((2, W, W), jnp.bfloat16),
            pltpu.VMEM((2, W, W), jnp.bfloat16),
            pltpu.VMEM((2, W, W), jnp.bfloat16),
            pltpu.VMEM((2, W, W), jnp.bfloat16),
            pltpu.VMEM((2, 8, 128), jnp.float32),
            pltpu.VMEM((NEAR, RHS, W), jnp.bfloat16),
            [pltpu.VMEM((row_span, strip, W), jnp.bfloat16)] * sources,
            [[pltpu.VMEM((2, strip, W), jnp.bfloat16)] * (col_bits + 1)] * streams,
            [pltpu.VMEM((W, W), jnp.bfloat16)] * streams,
            pltpu.VMEM(right_sides.shape[1:], jnp.float32),
            pltpu.VMEM((strips, strip, W), jnp.bfloat16),
            pltpu.SemaphoreType.DMA((5,)),
            pltpu.SemaphoreType.DMA((2,)),
            pltpu.SemaphoreType.DMA((1,)),
            pltpu.SemaphoreType.DMA((messages,)),
            pltpu.SemaphoreType.DMA((handed,)),
            pltpu.SemaphoreType.DMA((handed,)),
            pltpu.SemaphoreType.DMA((1,)),
            pltpu.SemaphoreType.DMA((spread_count,)),
        ],
        compiler_params=pltpu.CompilerParams(collective_id=0, has_side_effects=True),
        name="tree_solve",
    )(
        right_sides,
        lower_inverse,
        upper_inverse,
        lower_blocks,
        upper_blocks,
        node_widths,
        far_levels,
        owner_level,
    )


def solution(mesh):
    spans = tuple(mesh.shape[axis] for axis in AXES)
    split = P(AXES)
    return jax.shard_map(
        functools.partial(local, spans),
        mesh=mesh,
        in_specs=(split,) * 7 + (P(),),
        out_specs=split,
        check_vma=False,
    )
```

```python
import functools

import jax
import jax.numpy as jnp
from jax import lax
from jax.experimental import pallas as pl
from jax.experimental.pallas import tpu as pltpu
from jax.sharding import PartitionSpec as P

W = 256
RHS = 16
NB = 2
LOCAL_LEVELS = 2
LOCAL_COUNT = 3
OWN = LOCAL_COUNT
AXES = ("gz", "row", "col")


def flip_bits(coord, mask):
    flipped = coord
    bit = 1
    while bit <= mask:
        if mask & bit:
            flipped = flipped + bit - 2 * bit * lax.rem(lax.div(coord, bit), 2)
        bit *= 2
    return flipped


def exchange_plan(bits):
    phases = []
    for low in range(0, len(bits), 4):
        offsets = [0]
        for bit in bits[low : low + 4]:
            offsets += [offset + (1 << bit) for offset in offsets]
        phases.append(offsets[:0:-1])
    return phases


def times(vectors, matrix):
    return lax.dot_general(
        vectors, matrix, (((1,), (1,)), ((), ())), preferred_element_type=jnp.float32
    )


def half(values):
    return values.astype(jnp.bfloat16)


NEAR_BITS = 2
NEAR = 2**NEAR_BITS
CHAIN, TOP_SOLVE, SUB_SOLVE, BACK = range(4)
SOURCES = {CHAIN: 0, TOP_SOLVE: 1, SUB_SOLVE: 1, BACK: 2}


def kernel(
    spans,
    plans,
    down_plans,
    rights_hbm,
    lower_inverse_hbm,
    upper_inverse_hbm,
    lower_blocks_hbm,
    upper_blocks_hbm,
    widths_ref,
    far_ref,
    owner_ref,
    out_hbm,
    rights,
    lower_inverse,
    upper_inverse,
    lower_blocks,
    upper_blocks,
    outgoing,
    incoming,
    fused,
    near_blocks,
    far_blocks,
    second,
    beside_near,
    ahead,
    fars,
    bases,
    scattered,
    doubled,
    whole,
    solved_slots,
    sent_strips,
    load_sems,
    store_sems,
    send_sems,
    recv_sems,
    bulk_send_sems,
    bulk_recv_sems,
    spread_send_sems,
    spread_recv_sems,
):
    layer_span, row_span, col_span = spans
    col_bits = col_span.bit_length() - 1
    layer_size = row_span * col_span
    upper_levels = len(plans)
    top, sub = upper_levels, upper_levels - 1
    layer_at = lax.axis_index("gz")
    row_at = lax.axis_index("row")
    col_at = lax.axis_index("col")
    device = (layer_at * row_span + row_at) * col_span + col_at

    def peer(offset):
        return (
            flip_bits(layer_at, offset // layer_size),
            flip_bits(row_at, offset // col_span % row_span),
            flip_bits(col_at, offset % col_span),
        )

    pieces = [
        (rights_hbm.at[0], rights),
        (lower_inverse_hbm.at[0], lower_inverse),
        (lower_blocks_hbm.at[0], lower_blocks),
        (upper_blocks_hbm.at[0], upper_blocks),
        (upper_inverse_hbm.at[0], upper_inverse),
    ]
    loads = [
        pltpu.make_async_copy(source, target, load_sems.at[at])
        for at, (source, target) in enumerate(pieces)
    ]
    for load in loads:
        load.start()

    barrier = pltpu.get_barrier_semaphore()
    partners = {offset for plan in plans + down_plans for phase in plan for offset in phase}
    partners = sorted(partners | {step * col_span for step in range(1, row_span)})
    for offset in partners:
        pl.semaphore_signal(
            barrier, inc=1, device_id=peer(offset), device_id_type=pl.DeviceIdType.MESH
        )

    columns = lax.broadcasted_iota(jnp.int32, (RHS, W), 1)

    def spread(scalar):
        return jnp.full((RHS, W), scalar, jnp.int32)

    inside = [columns < widths_ref[0, slot] for slot in range(LOCAL_COUNT + 1)]
    far = [spread(far_ref[0, slot]) for slot in range(LOCAL_COUNT + 1)]
    my_level_scalar = owner_ref[device]
    my_level = spread(my_level_scalar)
    zeros = jnp.zeros((RHS, W), jnp.float32)

    steps = []
    for bit in range(upper_levels):
        size = 1 << bit
        steps.append(size - 2 * size * lax.rem(lax.div(device, size), 2))

    def level_at(offset):
        at = device
        for bit in range(upper_levels):
            if offset >> bit & 1:
                at = at + steps[bit]
        return owner_ref[at]

    def padded(slot, values):
        return jnp.where(inside[slot], values, 0.0)

    counts = [0, 0, 0]
    sends = []

    class Joined:
        def __init__(self, target, send_sem, recv_sem):
            self.sent = pltpu.make_async_copy(target, target, send_sem)
            self.arrived = pltpu.make_async_copy(target, target, recv_sem)

        def wait_recv(self):
            self.arrived.wait()

        def wait_send(self):
            self.sent.wait()

    def launch(rounded, phase):
        outbox, amount = counts[0], len(rounded)
        counts[0] += amount
        for index, part in enumerate(rounded):
            outgoing[outbox + index] = part
        begin, message = counts[1], counts[2]
        counts[1] += amount * len(phase)
        counts[2] += 1
        for index, offset in enumerate(phase):
            pltpu.make_async_remote_copy(
                src_ref=outgoing.at[pl.ds(outbox, amount)],
                dst_ref=incoming.at[pl.ds(begin + index * amount, amount)],
                send_sem=send_sems.at[0],
                recv_sem=recv_sems.at[message],
                device_id=peer(offset),
                device_id_type=pl.DeviceIdType.MESH,
            ).start()
        copy = Joined(
            incoming.at[pl.ds(begin, amount * len(phase))],
            send_sems.at[0],
            recv_sems.at[message],
        )
        copies = [(copy, begin + index * amount) for index in range(len(phase))]
        sends.append(copies[0])
        return copies

    bulk = {}
    spreads = []
    strips_sent = [0]
    vectors_sent = [0]

    groups = ["near", "second", "far", "ahead", "beside", "fars", "base"]
    joint = {
        "ahead": ahead.at[1],
        "beside": beside_near.at[1],
        "base": bases.at[pl.ds(1, NEAR - 1)],
    }

    def drain():
        blocks = fused.at[pl.ds(0, 5)]
        vectors = bases.at[pl.ds(1, NEAR - 1)]
        pltpu.make_async_copy(blocks, blocks, bulk_send_sems.at[0]).wait()
        pltpu.make_async_copy(fars.at[1], fars.at[1], bulk_send_sems.at[1]).wait()
        pltpu.make_async_copy(vectors, vectors, bulk_send_sems.at[2]).wait()
        pltpu.make_async_copy(incoming, incoming, send_sems.at[0]).wait()
        pltpu.make_async_copy(sent_strips, sent_strips, spread_send_sems.at[0]).wait()

    stores = []

    def store_out(slots):
        store = pltpu.make_async_copy(
            solved_slots.at[slots], out_hbm.at[0, slots], store_sems.at[len(stores)]
        )
        store.start()
        stores.append(store)

    def hand_out(name, source, target, offset):
        group = name if isinstance(name, str) else name[0]
        at = groups.index(group)
        pltpu.make_async_remote_copy(
            src_ref=source,
            dst_ref=target,
            send_sem=bulk_send_sems.at[max(at - 4, 0)],
            recv_sem=bulk_recv_sems.at[at],
            device_id=peer(offset),
            device_id_type=pl.DeviceIdType.MESH,
        ).start()
        extent = joint.get(group, target)
        bulk[name] = pltpu.make_async_copy(extent, extent, bulk_recv_sems.at[at])

    received = set()

    def await_bulk(name):
        group = name if isinstance(name, str) else name[0]
        if group not in received:
            received.add(group)
            bulk[name].wait()

    def exchange(values, plan, narrow, besides, started=None):
        for index, phase in enumerate(plan):
            rounded = [half(value) for value in values]
            copies = started if started and index == 0 else launch(rounded, phase)
            if index < len(besides):
                besides[index]()
            if narrow:
                values = [part.astype(jnp.float32) for part in rounded]
            copies[0][0].wait_recv()
            for _, at in copies:
                values = [
                    value + incoming[at + part].astype(jnp.float32)
                    for part, value in enumerate(values)
                ]
        return values

    strip = W // row_span
    my_strip = pl.ds(pl.multiple_of(row_at * strip, strip), strip)
    stream_level = {CHAIN: sub, TOP_SOLVE: top, SUB_SOLVE: sub, BACK: sub}
    spread_waits = {}

    def spread_copies(key, pairs, extent):
        at = len(spreads)
        for source, target, offset in pairs:
            pltpu.make_async_remote_copy(
                src_ref=source,
                dst_ref=target,
                send_sem=spread_send_sems.at[0],
                recv_sem=spread_recv_sems.at[at],
                device_id=peer(offset),
                device_id_type=pl.DeviceIdType.MESH,
            ).start()
        strips_sent[0] += len(pairs)
        copy = Joined(extent, spread_send_sems.at[0], spread_recv_sems.at[at])
        spreads.append(copy)
        spread_waits[key] = [copy]

    def await_spread(key):
        for copy in spread_waits.pop(key, ()):
            copy.wait_recv()

    held = {}
    for level in (sub, top):
        place = jnp.int32(0)
        known_here = []
        here = jnp.int32(1)
        layers = (0,) if level == sub else (0, layer_size)
        rounds = [(0, 1)] + [(1 << bit, 2 << bit) for bit in range(col_bits)]
        for layer in layers:
            for low, high in rounds if layer == layers[-1] else rounds[:1]:
                for others in layers if low else (layer,):
                    for step in range(row_span):
                        for offset in range(low, high):
                            found = level_at(others + step * col_span + offset) == level
                            here = jnp.where(found, 0, here)
                            if layer == others == low == 0:
                                place = jnp.where(found, step, place)
                known_here.append(here)
        held[level] = (place, known_here)

    def reach_of(stream, stage):
        if stream == TOP_SOLVE:
            return 1 << stage - 1 if stage else layer_size
        return 1 << stage

    others = pl.ds(1, row_span - 1)

    def scatter_rows(source, matrix):
        pairs = []
        for step in range(1, row_span):
            start = pl.multiple_of(flip_bits(row_at, step) * strip, strip)
            rows = matrix.at[pl.ds(start, strip)]
            pairs.append((rows, scattered[source].at[step], step * col_span))
        spread_copies(("scatter", source), pairs, scattered[source].at[others])
        scattered[source][0] = matrix[my_strip]

    def merged(stream, stage):
        place, known_here = held[stream_level[stream]]
        if stage == 0:
            await_spread(("scatter", SOURCES[stream]))
            return scattered[SOURCES[stream]][place]
        await_spread(("double", stream, stage - 1))
        return doubled[stream][stage - 1][known_here[stage - 1]]

    def double_cols(stream, stage):
        mine, theirs = (doubled[stream][stage].at[side] for side in range(2))
        doubled[stream][stage][0] = merged(stream, stage)
        pairs = [(mine, theirs, reach_of(stream, stage))]
        spread_copies(("double", stream, stage), pairs, theirs)

    def gather_rows(stream, stage):
        whole[stream][my_strip] = merged(stream, stage)
        rows = whole[stream].at[my_strip]
        pairs = [(rows, rows, step * col_span) for step in range(1, row_span)]
        extent = whole[stream].at[pl.ds(0, strip * (row_span - 1))]
        spread_copies(("gather", stream), pairs, extent)

    pending = [None] + [zeros for _ in range(upper_levels)]

    def scatter_up(product, slot, height):
        for level in range(1, upper_levels + 1):
            pending[level] = pending[level] + jnp.where(
                far[slot] == level + LOCAL_LEVELS - 1 - height, product, 0.0
            )

    forward = [None] * (LOCAL_COUNT + 1)
    loads[0].wait()
    loads[1].wait()
    for slot in range(2):
        forward[slot] = padded(slot, times(half(rights[slot]), lower_inverse[slot]))
    loads[2].wait()
    near = times(half(forward[0]), lower_blocks[0, 0]) + times(
        half(forward[1]), lower_blocks[1, 0]
    )
    for slot in range(2):
        scatter_up(times(half(forward[slot]), lower_blocks[slot, 1]), slot, 0)
    forward[2] = padded(2, times(half(rights[2] - near), lower_inverse[2]))
    pending[1] = pending[1] + times(half(forward[2]), lower_blocks[2, 0])
    scatter_up(times(half(forward[2]), lower_blocks[2, 1]), 2, 1)
    for level in range(1, upper_levels + 1):
        pending[level] = pending[level] - jnp.where(my_level == level, rights[OWN], 0.0)

    wide_columns = lax.broadcasted_iota(jnp.int32, (W, W), 1)
    wide_rows = lax.broadcasted_iota(jnp.int32, (W, W), 0)

    def own_columns(matrix):
        kept = jnp.where(
            wide_columns < widths_ref[0, OWN], matrix.astype(jnp.float32), 0.0
        )
        return half(kept)

    def own_rows(matrix):
        return jnp.where(wide_rows < widths_ref[0, OWN], matrix, 0.0)

    def lower_product(block_id):
        return jnp.dot(
            own_columns(lower_blocks[OWN, block_id]),
            lower_inverse[OWN],
            preferred_element_type=jnp.float32,
        )

    def upper_product(slot, block_id):
        return jnp.dot(
            upper_inverse[slot], upper_blocks[slot, block_id], preferred_element_type=jnp.float32
        )

    def split_times(values, matrix):
        large = half(values)
        small = half(values - large.astype(jnp.float32))
        return times(large, matrix) + times(small, matrix)

    far_is_near = jnp.full((W, W), far_ref[0, OWN], jnp.int32) == 1

    far_product = lower_product(1)
    fused[0] = half(lower_product(0) + jnp.where(far_is_near, far_product, 0.0))
    beside_near[0] = fused[0]
    fused[1] = half(far_product)
    loads[3].wait()
    loads[4].wait()
    fused[2] = half(
        own_rows(
            jnp.dot(
                own_columns(upper_inverse[OWN]),
                lower_inverse[OWN],
                preferred_element_type=jnp.float32,
            )
        )
    )
    far_product = own_rows(upper_product(OWN, 1))
    far_blocks[0] = half(far_product)
    near_blocks[0] = half(
        own_rows(upper_product(OWN, 0)) + jnp.where(far_is_near, far_product, 0.0)
    )
    ahead[0] = near_blocks[0]
    fars[0] = far[OWN][: fars.shape[1], : fars.shape[2]].astype(jnp.float32)

    pl.semaphore_wait(barrier, len(partners))

    own_base = [zeros]
    residue = [None]

    def own_solve(level):
        solved = times(residue[0], fused[2])
        own_base[0] = own_base[0] + jnp.where(my_level == level, solved, 0.0)

    def far_up(level):
        product = jnp.where(my_level == level, times(residue[0], fused[1]), 0.0)
        for target in range(level + 2, upper_levels + 1):
            pending[target] = pending[target] + jnp.where(
                far[OWN] == target - level, product, 0.0
            )

    def leaf_products(slot):
        for block_id in range(NB):
            fused[3 + 2 * slot + block_id] = half(upper_product(slot, block_id))
        if slot == 2:
            kept = half(
                jnp.where(
                    wide_rows < widths_ref[0, 2], fused[3 + 2 * 2].astype(jnp.float32), 0.0
                )
            )
            for leaf in range(2):
                fused[9 + leaf] = half(
                    jnp.dot(
                        fused[3 + 2 * leaf], kept, preferred_element_type=jnp.float32
                    )
                )

    leaf_base = [None] * LOCAL_COUNT

    def first_round():
        scatter_rows(0, fused.at[0])
        scatter_rows(1, fused.at[2])
        scatter_rows(2, near_blocks.at[0])
        hand_ahead(0)
        hand_out("near", near_blocks.at[0], near_blocks.at[1], 1)

    near_levels = [level_at(offset) for offset in range(NEAR)]
    halves = {}

    def hand_ahead(part):
        rows = pl.ds(part * (W // 2), W // 2)
        hand_out(("ahead", part), near_blocks.at[0, rows], ahead.at[1, rows], 2)

    def hand_beside(part):
        rows = pl.ds(part * (W // 2), W // 2)
        hand_out(
            ("beside", part), fused.at[0, rows], beside_near.at[1, rows], col_span
        )

    def beside_up(level):
        if level == 1:
            first_round()
            return
        if level == 2:
            hand_ahead(1)
        if level == sub - 1:
            hand_beside(1)
        if level < sub:
            double_cols(CHAIN, level - 2)
            if level > 2:
                double_cols(BACK, level - 3)
            if level == 2:
                double_cols(TOP_SOLVE, 0)
            double_cols(SUB_SOLVE, level - 2)
            if level == 2:
                hand_beside(0)
            double_cols(TOP_SOLVE, level - 1)
            if level == sub - 1:
                double_cols(BACK, level - 2)
        own_solve(level - 1)
        if level == sub:
            gather_rows(CHAIN, col_bits)
            gather_rows(SUB_SOLVE, col_bits)
            gather_rows(TOP_SOLVE, col_bits + 1)
            gather_rows(BACK, col_bits)
            await_bulk(("ahead", 0))
            await_bulk(("ahead", 1))
            second[0] = ahead[ahead_place]
            hand_out("second", second.at[0], second.at[1], 1)
            hand_out("far", far_blocks.at[0], far_blocks.at[1], 1)
            hand_out("fars", fars.at[0], fars.at[1], 1)
        if level - 2 < LOCAL_COUNT:
            leaf_products(level - 2)

    ahead_place = jnp.where(near_levels[2] == 2, 1, 0)
    second_place = jnp.where(near_levels[1] == 2, 1, jnp.where(near_levels[3] == 2, 1, 0))

    def holder(level):
        offset_of = jnp.int32(0)
        for offset in range(2**level):
            offset_of = jnp.where(near_levels[offset] == level, offset, offset_of)
        return offset_of

    for level in range(1, sub):
        if level == sub - 1:
            for copy, at in launch([half(pending[sub])], [col_span]):
                halves["copy"], halves["at"] = copy, at
        gathered = exchange(
            [pending[level]], plans[level - 1], False, [functools.partial(beside_up, level)]
        )[0]
        residue[0] = half(-gathered)
        if level < sub - 1:
            product = times(residue[0], fused[0])
            pending[level + 1] = pending[level + 1] + jnp.where(
                my_level == level, product, 0.0
            )
            far_up(level)

    across = level_at(col_span)
    on_side = jnp.where(across == sub - 1, 1, 0)
    here = spread(jnp.where(my_level_scalar == sub - 1, 1, on_side)) == 1
    halves["copy"].wait_recv()
    far_up(sub - 1)
    await_bulk(("beside", 0))
    await_bulk(("beside", 1))
    product = times(residue[0], beside_near[on_side])
    value = (
        pending[sub]
        + incoming[halves["at"]].astype(jnp.float32)
        + jnp.where(here, product, 0.0)
    )
    layer_plan = down_plans[-1]

    def beside_sub():
        halves["layer"] = launch([half(pending[top])], layer_plan[0])
        beside_up(sub)

    sums = exchange([value], plans[sub - 1], False, [beside_sub])
    sub_residue = half(-sums[0])
    await_spread(("gather", CHAIN))
    chained = times(sub_residue, whole[CHAIN][...])
    layer_sum = exchange([pending[top]], layer_plan, False, [], halves["layer"])[0] + chained
    sub_base = [None]

    def beside_top():
        await_spread(("gather", SUB_SOLVE))
        sub_base[0] = times(sub_residue, whole[SUB_SOLVE][...])
        for slot in range(LOCAL_COUNT):
            leaf_base[slot] = split_times(forward[slot], upper_inverse[slot])
        await_spread(("gather", TOP_SOLVE))
        await_spread(("gather", BACK))

    total = exchange([layer_sum], plans[top - 1], False, [beside_top])[0]

    known = [None] * (upper_levels + 1)

    def pick(slot, below, lowest):
        chosen = zeros
        for level in range(lowest, upper_levels + 1):
            chosen = chosen + jnp.where(far[slot] == level - below, known[level], 0.0)
        return half(chosen)

    solved = times(half(-total), whole[TOP_SOLVE][...])
    own_solution = jnp.where(my_level == top, solved, 0.0)
    known[top] = half(solved).astype(jnp.float32)
    solved = sub_base[0] - times(half(solved), whole[BACK][...])
    own_solution = own_solution + jnp.where(my_level == sub, solved, 0.0)
    known[sub] = half(solved).astype(jnp.float32)

    for level in range(sub - 1, NEAR_BITS, -1):
        chosen = zeros
        for target in range(level + 1, upper_levels + 1):
            chosen = chosen + jnp.where(my_level + far[OWN] == target, known[target], 0.0)
        base = own_base[0] - times(half(chosen), far_blocks[0])
        solved = base - times(half(known[level + 1]), near_blocks[0])
        solved = jnp.where(my_level == level, solved, 0.0)
        own_solution = own_solution + solved

        def beside_down():
            if level == NEAR_BITS + 1:
                bases[0] = half(jnp.where(my_level == 1, own_base[0], base))
                for offset in range(1, NEAR):
                    hand_out(("base", offset), bases.at[0], bases.at[offset], offset)
                for name in bulk:
                    if name[0] != "base":
                        await_bulk(name)

        known[level] = exchange([solved], down_plans[level - 1], True, [beside_down])[0]
    for name in bulk:
        await_bulk(name)

    at = holder(1)
    reach = fars[at]
    reach = jnp.concatenate([reach] * (W // reach.shape[1]), axis=1)
    reach = jnp.concatenate([reach] * (RHS // reach.shape[0]), axis=0)
    chosen = zeros
    for target in range(3, upper_levels + 1):
        chosen = chosen + jnp.where(reach == float(target - 1), known[target], 0.0)
    base = bases[at].astype(jnp.float32) - times(half(chosen), far_blocks[at])
    solved = bases[holder(2)].astype(jnp.float32) - times(
        half(known[3]), second[second_place]
    )
    own_solution = own_solution + jnp.where(my_level == 2, solved, 0.0)
    known[2] = half(solved).astype(jnp.float32)
    solved = base - times(half(solved), near_blocks[at])
    own_solution = own_solution + jnp.where(my_level == 1, solved, 0.0)
    known[1] = half(solved).astype(jnp.float32)
    solved_slots[OWN] = own_solution
    store_out(pl.ds(OWN, 1))
    nearest = half(known[1])
    root_base = leaf_base[2] - times(pick(2, 0, 2), fused[3 + 2 * 2 + 1])
    solved_slots[2] = padded(2, root_base - times(nearest, fused[3 + 2 * 2]))
    root_part = half(padded(2, root_base))
    for slot in range(2):
        solved = leaf_base[slot] - times(pick(slot, -1, 1), fused[3 + 2 * slot + 1])
        solved = solved - times(root_part, fused[3 + 2 * slot])
        solved_slots[slot] = padded(slot, solved + times(nearest, fused[9 + slot]))

    store_out(pl.ds(0, 3))
    drain()
    for store in stores:
        store.wait()


def local(
    spans,
    right_sides,
    lower_inverse,
    upper_inverse,
    lower_blocks,
    upper_blocks,
    node_widths,
    far_levels,
    owner_level,
):
    layer_span, row_span, col_span = spans
    upper_levels = (layer_span * row_span * col_span).bit_length() - 1
    col_bits = col_span.bit_length() - 1
    top, sub = upper_levels, upper_levels - 1
    plans = [exchange_plan(list(range(level))) for level in range(1, sub)]
    plans.append(exchange_plan(list(range(col_bits)) + [sub - 1]))
    plans.append(exchange_plan([sub]))
    down_plans = [[]] * NEAR_BITS
    down_plans += [exchange_plan(list(range(level))) for level in range(NEAR_BITS + 1, sub)]
    down_plans.append(exchange_plan(list(range(sub))))
    vectors = [1] * (sub + 2 + len(down_plans))
    routes = list(zip(vectors, plans + [[[col_span]]] + down_plans))
    phases = sum(amount * len(plan) for amount, plan in routes)
    messages = sum(len(plan) for _, plan in routes)
    boxes = sum(amount * len(phase) for amount, plan in routes for phase in plan)
    streams, sources = len(SOURCES), len(set(SOURCES.values()))
    strip = W // row_span
    strips = (sources + streams) * (row_span - 1) + streams * col_bits + 1
    spread_count = sources + streams * (col_bits + 1) + 1
    hbm = pl.BlockSpec(memory_space=pl.ANY)
    smem = pl.BlockSpec(memory_space=pltpu.SMEM)
    return pl.pallas_call(
        functools.partial(kernel, spans, plans, down_plans),
        out_shape=jax.ShapeDtypeStruct(right_sides.shape, jnp.float32),
        in_specs=[hbm] * 5 + [smem] * 3,
        out_specs=hbm,
        scratch_shapes=[
            pltpu.VMEM(right_sides.shape[1:], jnp.float32),
            pltpu.VMEM(lower_inverse.shape[1:], jnp.bfloat16),
            pltpu.VMEM(upper_inverse.shape[1:], jnp.bfloat16),
            pltpu.VMEM(lower_blocks.shape[1:], jnp.bfloat16),
            pltpu.VMEM(upper_blocks.shape[1:], jnp.bfloat16),
            pltpu.VMEM((phases, RHS, W), jnp.bfloat16),
            pltpu.VMEM((boxes, RHS, W), jnp.bfloat16),
            pltpu.VMEM((5 + NB * LOCAL_COUNT, W, W), jnp.bfloat16),
            pltpu.VMEM((2, W, W), jnp.bfloat16),
            pltpu.VMEM((2, W, W), jnp.bfloat16),
            pltpu.VMEM((2, W, W), jnp.bfloat16),
            pltpu.VMEM((2, W, W), jnp.bfloat16),
            pltpu.VMEM((2, W, W), jnp.bfloat16),
            pltpu.VMEM((2, 8, 128), jnp.float32),
            pltpu.VMEM((NEAR, RHS, W), jnp.bfloat16),
            [pltpu.VMEM((row_span, strip, W), jnp.bfloat16)] * sources,
            [[pltpu.VMEM((2, strip, W), jnp.bfloat16)] * (col_bits + 1)] * streams,
            [pltpu.VMEM((W, W), jnp.bfloat16)] * streams,
            pltpu.VMEM(right_sides.shape[1:], jnp.float32),
            pltpu.VMEM((strips, strip, W), jnp.bfloat16),
            pltpu.SemaphoreType.DMA((5,)),
            pltpu.SemaphoreType.DMA((2,)),
            pltpu.SemaphoreType.DMA((1,)),
            pltpu.SemaphoreType.DMA((messages,)),
            pltpu.SemaphoreType.DMA((3,)),
            pltpu.SemaphoreType.DMA((7,)),
            pltpu.SemaphoreType.DMA((1,)),
            pltpu.SemaphoreType.DMA((spread_count,)),
        ],
        compiler_params=pltpu.CompilerParams(collective_id=0, has_side_effects=True),
        name="tree_solve",
    )(
        right_sides,
        lower_inverse,
        upper_inverse,
        lower_blocks,
        upper_blocks,
        node_widths,
        far_levels,
        owner_level,
    )


def solution(mesh):
    spans = tuple(mesh.shape[axis] for axis in AXES)
    split = P(AXES)
    return jax.shard_map(
        functools.partial(local, spans),
        mesh=mesh,
        in_specs=(split,) * 7 + (P(),),
        out_specs=split,
        check_vma=False,
    )
```
